32 devices in a mesh: fsdp: 32 (over z, y, x, core).
Axes of the slice: x: 2, y: 2, z: 4, core: 2. Of those that a mesh axis runs over, the one named last changes fastest.
Arguments:
- timesteps: float32 [16384], P('fsdp')
- guidance: float32 [16384], P('fsdp')
- pooled: bfloat16 [16384, 2048], P('fsdp')
- time_w1: bfloat16 [256, 1152], replicated
- time_b1: bfloat16 [1152], replicated
- time_w2: bfloat16 [1152, 1152], replicated
- time_b2: bfloat16 [1152], replicated
- guide_w1: bfloat16 [256, 1152], replicated
- guide_b1: bfloat16 [1152], replicated
- guide_w2: bfloat16 [1152, 1152], replicated
- guide_b2: bfloat16 [1152], replicated
- text_w1: bfloat16 [2048, 1152], replicated
- text_b1: bfloat16 [1152], replicated
- text_w2: bfloat16 [1152, 1152], replicated
- text_b2: bfloat16 [1152], replicated
- w_mod: bfloat16 [1152, 5760], P(None, 'fsdp')
- b_mod: bfloat16 [5760], P('fsdp')
- d_mods: bfloat16 [16384, 5760], P('fsdp')
Outputs:
- output 1: bfloat16 [16384, 5760], P('fsdp')
- output 2: float32 [1152, 5760], P(None, 'fsdp')
- output 3: float32 [5760], P('fsdp')
- output 4: float32 [256, 1152], replicated
- output 5: float32 [1152], replicated
- output 6: float32 [1152, 1152], replicated
- output 7: float32 [1152], replicated
- output 8: float32 [256, 1152], replicated
- output 9: float32 [1152], replicated
- output 10: float32 [1152, 1152], replicated
- output 11: float32 [1152], replicated
- output 12: float32 [2048, 1152], replicated
- output 13: float32 [1152], replicated
- output 14: float32 [1152, 1152], replicated
- output 15: float32 [1152], replicated
All inputs are finite; a program needn't handle non-finite values.
Results may differ from the reference program's by a relative error of at most 0.00486957.
Values are sent between devices in bfloat16 or wider.
A program may use at most 1 GiB of HBM per device.

```python
import math
import jax
import jax.numpy as jnp

GLOBAL_BATCH = 16384
HIDDEN = 1152
POOL_WIDTH = 2048
FREQ_WIDTH = 256
MOD_WIDTH = 5760


def setup_inputs(seed: int = 0) -> dict:
    key_list = jax.random.split(jax.random.key(seed), 18)

    def draw_weight(sub_key, fan_in, fan_out):
        return (jax.random.normal(sub_key, (fan_in, fan_out), jnp.float32) * fan_in ** -0.5).astype(jnp.bfloat16)

    def draw_bias(sub_key, fan_out):
        return (0.5 * jax.random.normal(sub_key, (fan_out,), jnp.float32)).astype(jnp.bfloat16)

    grad_scale = GLOBAL_BATCH ** -0.5
    return dict(
        timesteps=jax.random.uniform(key_list[0], (GLOBAL_BATCH,), jnp.float32),
        guidance=jax.random.uniform(key_list[1], (GLOBAL_BATCH,), jnp.float32, 1.0, 5.0),
        pooled=jax.random.normal(key_list[2], (GLOBAL_BATCH, POOL_WIDTH), jnp.float32).astype(jnp.bfloat16),
        time_w1=draw_weight(key_list[3], FREQ_WIDTH, HIDDEN),
        time_b1=draw_bias(key_list[4], HIDDEN),
        time_w2=draw_weight(key_list[5], HIDDEN, HIDDEN),
        time_b2=draw_bias(key_list[6], HIDDEN),
        guide_w1=draw_weight(key_list[7], FREQ_WIDTH, HIDDEN),
        guide_b1=draw_bias(key_list[8], HIDDEN),
        guide_w2=draw_weight(key_list[9], HIDDEN, HIDDEN),
        guide_b2=draw_bias(key_list[10], HIDDEN),
        text_w1=draw_weight(key_list[11], POOL_WIDTH, HIDDEN),
        text_b1=draw_bias(key_list[12], HIDDEN),
        text_w2=draw_weight(key_list[13], HIDDEN, HIDDEN),
        text_b2=draw_bias(key_list[14], HIDDEN),
        w_mod=draw_weight(key_list[15], HIDDEN, MOD_WIDTH),
        b_mod=draw_bias(key_list[16], MOD_WIDTH),
        d_mods=(jax.random.normal(key_list[17], (GLOBAL_BATCH, MOD_WIDTH), jnp.float32) * grad_scale).astype(jnp.bfloat16),
    )


def sinusoid(values):
    half_width = FREQ_WIDTH // 2
    freq_table = jnp.exp(-math.log(10000.0) * jnp.arange(half_width, dtype=jnp.float32) / half_width)
    angles = (1000.0 * values)[:, None] * freq_table[None, :]
    return jnp.concatenate([jnp.cos(angles), jnp.sin(angles)], axis=1).astype(jnp.bfloat16)


def silu_grad(values):
    sigmoid_v = jax.nn.sigmoid(values)
    return sigmoid_v * (1.0 + values * (1.0 - sigmoid_v))


def mlp_forward(inputs_bf, params):
    hidden = jnp.dot(inputs_bf, params[0], preferred_element_type=jnp.float32) + params[1].astype(jnp.float32)
    act_bf = jax.nn.silu(hidden).astype(jnp.bfloat16)
    output = jnp.dot(act_bf, params[2], preferred_element_type=jnp.float32) + params[3].astype(jnp.float32)
    return output, hidden, act_bf


def mlp_backward(inputs_bf, params, hidden, act_bf, d_out, d_out_bf):
    grad_w2 = jnp.dot(act_bf.T, d_out_bf, preferred_element_type=jnp.float32)
    grad_b2 = jnp.sum(d_out, axis=0)
    d_act = jnp.dot(d_out_bf, params[2].T, preferred_element_type=jnp.float32)
    d_hidden = d_act * silu_grad(hidden)
    grad_w1 = jnp.dot(inputs_bf.T, d_hidden.astype(jnp.bfloat16), preferred_element_type=jnp.float32)
    grad_b1 = jnp.sum(d_hidden, axis=0)
    return grad_w1, grad_b1, grad_w2, grad_b2


def reference(timesteps, guidance, pooled, time_w1, time_b1, time_w2, time_b2, guide_w1, guide_b1, guide_w2, guide_b2, text_w1, text_b1, text_w2, text_b2, w_mod, b_mod, d_mods):
    inputs_list = [sinusoid(timesteps), sinusoid(guidance), pooled]
    params_list = [(time_w1, time_b1, time_w2, time_b2), (guide_w1, guide_b1, guide_w2, guide_b2), (text_w1, text_b1, text_w2, text_b2)]
    saved_acts = [mlp_forward(inputs_bf, params) for inputs_bf, params in zip(inputs_list, params_list)]
    cond_vec = saved_acts[0][0] + saved_acts[1][0] + saved_acts[2][0]
    cond_silu = jax.nn.silu(cond_vec).astype(jnp.bfloat16)
    modulation = (jnp.dot(cond_silu, w_mod, preferred_element_type=jnp.float32) + b_mod.astype(jnp.float32)).astype(jnp.bfloat16)
    grad_wmod = jnp.dot(cond_silu.T, d_mods, preferred_element_type=jnp.float32)
    grad_bmod = jnp.sum(d_mods, axis=0, dtype=jnp.float32)
    d_cond = jnp.dot(d_mods, w_mod.T, preferred_element_type=jnp.float32)
    d_vec = d_cond * silu_grad(cond_vec)
    d_vec_bf = d_vec.astype(jnp.bfloat16)
    time_grads = mlp_backward(inputs_list[0], params_list[0], saved_acts[0][1], saved_acts[0][2], d_vec, d_vec_bf)
    guide_grads = mlp_backward(inputs_list[1], params_list[1], saved_acts[1][1], saved_acts[1][2], d_vec, d_vec_bf)
    text_grads = mlp_backward(inputs_list[2], params_list[2], saved_acts[2][1], saved_acts[2][2], d_vec, d_vec_bf)
    return (modulation, grad_wmod, grad_bmod, time_grads[0], time_grads[1], time_grads[2], time_grads[3], guide_grads[0], guide_grads[1], guide_grads[2], guide_grads[3], text_grads[0], text_grads[1], text_grads[2], text_grads[3])
```

```python
import functools
import math
import jax
import jax.numpy as jnp
from jax import lax
from jax.experimental import pallas as pl
from jax.experimental.pallas import tpu as pltpu
from jax.sharding import PartitionSpec as P

AXIS = "fsdp"
MESH = pl.DeviceIdType.MESH
MAX_PERIOD = 10000.0
TIME_SCALE = 1000.0
CONTRACT_ROWS = (((0,), (0,)), ((), ()))
CONTRACT_COLS = (((1,), (1,)), ((), ()))
F32, BF16 = jnp.float32, jnp.bfloat16
VMEM_LIMIT = 62 << 20
TWO, ZS, CHIPS, DEVICES = 2, 4, 16, 32
ROWS, WIDTH, MOD, SHARE, PADDED = 512, 1152, 5760, 180, 184
TILE, TILES = 384, 15
Z_ORDER = (3, 0, 2, 1)
ANY = pl.BlockSpec(memory_space=pl.ANY)
IN_VMEM = pl.BlockSpec(memory_space=pltpu.VMEM)
DMA = pltpu.SemaphoreType.DMA
WMOD_SPLIT = (80, 64, 16, 24)
WGRAD_SPLIT = (72, 72, 24, 16)
EMBED_SPLIT = (80, 72, 24, 16)


class Peers:
    def __init__(self):
        me = lax.axis_index(AXIS)
        bits = []
        for _ in range(3):
            bits.append(lax.rem(me, TWO))
            me = lax.div(me, TWO)
        self.c, self.x, self.y = bits
        self.oc, self.ox, self.oy = (1 - bit for bit in bits)
        self.z = me
        self.core = self.device(me, self.y, self.x, self.oc)
        self.xn = self.device(me, self.y, self.ox, self.c)
        self.yn = self.device(me, self.oy, self.x, self.c)

    def device(self, z, y, x, c):
        return (((z * TWO + y) * TWO + x) * TWO + c,)

    def column(self, zp):
        return self.device(zp, self.y, self.x, self.c)

    def elsewhere(self, fn):
        for zp in range(ZS):
            pl.when(self.z != zp)(functools.partial(fn, zp))

    def barrier(self):
        sem = pltpu.get_barrier_semaphore()

        def greet(peer):
            pl.semaphore_signal(sem, device_id=peer, device_id_type=MESH)

        for peer in (self.core, self.xn, self.yn):
            greet(peer)
        self.elsewhere(lambda zp: greet(self.column(zp)))
        pl.semaphore_wait(sem, 6)


def remote(src, dst, sems, peer):
    pltpu.make_async_remote_copy(src_ref=src, dst_ref=dst, send_sem=sems[0], recv_sem=sems[1], device_id=peer, device_id_type=MESH).start()


def local(src, dst, sem):
    pltpu.make_async_copy(src, dst, sem).start()


def wait_for(ref, sem):
    pltpu.make_async_copy(ref, ref, sem).wait()


def add_rows(dst, src):
    if len(dst.shape) > TWO:
        for i in range(dst.shape[0]):
            add_rows(dst.at[i], src.at[i])
        return
    rows = dst.shape[0]
    step = 24 if rows % 24 == 0 else 8

    def body(i, carry):
        at = pl.ds(pl.multiple_of(i * step, 8), step)
        dst[at, :] = dst[at, :] + src[at, :]
        return carry

    lax.fori_loop(0, rows // step, body, 0)


class Sems:
    def __init__(self, refs, *index):
        self.send, self.recv, self.index = *refs, index

    def __getitem__(self, k):
        return self.send.at[(*self.index, k)], self.recv.at[(*self.index, k)]

    def under(self, k):
        return Sems((self.send, self.recv), *self.index, k)

    @staticmethod
    def scratch(*shape):
        return [DMA(shape), DMA(shape)]


class Split:
    def __init__(self, *n):
        starts = [sum(n[:i]) for i in range(ZS)]
        ranges = [pl.ds(start, size) for start, size in zip(starts, n)]
        self.n, self.colours = (n[:TWO], n[TWO:]), (ranges[:TWO], ranges[TWO:])
        self.a, self.b = sum(self.n[0]), sum(self.n[1])
        self.rows = self.a + self.b
        self.all_a, self.all_b = pl.ds(0, self.a), pl.ds(self.a, self.b)
        size = -(-self.a // DEVICES) * 8
        self.chunks = [pl.ds(at, min(size, self.a - at)) for at in range(0, self.a, size)]


class PlaneReduce:
    @staticmethod
    def shapes(sizes):
        one, two = sizes
        return [(TWO, one), (TWO, two), (one,), (two,)]

    def __init__(self, p, plane, colours, boxes, sems):
        one, two = colours
        x1, y1, y2, x2 = boxes
        self.sems = sems
        self.moves = (
            (plane.at[:, p.ox, one], x1, p.xn), (plane.at[p.oy, :, two], y1, p.yn),
            (plane.at[p.oy, p.x, one], y2, p.yn), (plane.at[p.y, p.ox, two], x2, p.xn),
        )
        mine = plane.at[p.y, p.x]
        self.first = ((x1.at[p.oy], x1.at[p.y]), (y1.at[p.ox], y1.at[p.x]))
        self.mine = (mine.at[one], mine.at[two])

    def send(self, k):
        src, dst, peer = self.moves[k]
        remote(src, dst, self.sems[k], peer)

    def got(self, k):
        wait_for(self.moves[k][1], self.sems[k][1])

    def start(self):
        for k in range(TWO):
            self.send(k)

    def middle(self):
        for k in range(TWO):
            self.got(k)
            add_rows(self.moves[k + TWO][0], self.first[k][0])
            self.send(k + TWO)
        for k in range(TWO):
            add_rows(self.mine[k], self.first[k][1])

    def end(self):
        for k in range(TWO):
            self.got(k + TWO)
            add_rows(self.mine[k], self.moves[k + TWO][1])

    def drain(self):
        for k, move in enumerate(self.moves):
            wait_for(move[1], self.sems[k][0])


class ReduceScatter:
    @staticmethod
    def scratch(s):
        whole = [(ZS, TWO, TWO, s.rows)] * TWO
        planes = [(ZS,) + shape for shape in PlaneReduce.shapes(s.n[0])] + PlaneReduce.shapes(s.n[1])
        shapes = whole + planes + [(TWO, ZS, s.a), (ZS, TWO, TWO, s.b)]
        buffers = [pltpu.VMEM(shape + (WIDTH,), F32) for shape in shapes]
        return buffers + [DMA((ZS,))] + Sems.scratch(ZS) + Sems.scratch(ZS, ZS) + Sems.scratch(TWO, ZS, len(s.chunks)) + Sems.scratch(ZS) + Sems.scratch(ZS)

    def __init__(self, p, sources, pieces, s, scratch):
        self.p, self.sources, self.pieces, self.s = p, sources, pieces, s
        scratch = list(scratch)
        take = lambda n: [scratch.pop(0) for _ in range(n)]
        self.part, self.fromc = take(TWO)
        boxes, slab_boxes = take(ZS), take(ZS)
        self.line, self.slabs, self.lsem = take(3)
        self.csems, plane_sems, self.zsems, self.bsems, slab_sems = (Sems(take(TWO)) for _ in range(5))
        self.planes = [PlaneReduce(p, self.part.at[zp], s.colours[0], [box.at[zp] for box in boxes], plane_sems.under(zp)) for zp in range(ZS)]
        self.slab = PlaneReduce(p, self.part.at[p.z], s.colours[1], slab_boxes, slab_sems)

    def begin(self, zp):
        p = self.p

        def load(core):
            mine = self.pieces[core]
            for src, start, n, at in self.pieces[1 - core]:
                remote(self.sources[src].at[zp, :, :, pl.ds(start, n)], self.fromc.at[zp, :, :, pl.ds(at, n)], self.csems[zp], p.core)
            for src, start, n, at in mine:
                local(self.sources[src].at[zp, :, :, pl.ds(start, n)], self.part.at[zp, :, :, pl.ds(at, n)], self.lsem.at[zp])

        for core in range(TWO):
            pl.when(p.c == core)(functools.partial(load, core))

    def both_cores(self, zp):
        wait_for(self.part.at[zp], self.lsem.at[zp])
        wait_for(self.fromc.at[zp], self.csems[zp][1])
        add_rows(self.part.at[zp], self.fromc.at[zp])

    def slab_out(self, zp):
        p = self.p

        @pl.when(p.z != zp)
        def _():
            sems = self.bsems[zp][0], self.bsems[p.z][1]
            remote(self.part.at[zp, :, :, self.s.all_b], self.slabs.at[p.z], sems, p.column(zp))

    def slab_sum(self, zp):
        wait_for(self.slabs.at[zp], self.bsems[zp][1])
        add_rows(self.part.at[self.p.z, :, :, self.s.all_b], self.slabs.at[zp])

    def line_in(self, way, zp, k, part):
        box = self.line.at[way, zp, part]
        wait_for(box, self.zsems.under(way).under(zp)[k][1])
        add_rows(self.part.at[zp, self.p.y, self.p.x, part], box)

    def hop(self, zp, distance):
        p = self.p

        def go(way, step):
            for k, part in enumerate(self.s.chunks):
                if distance:
                    self.line_in(way, zp, k, part)
                remote(self.part.at[zp, p.y, p.x, part], self.line.at[way, zp, part], self.zsems.under(way).under(zp)[k], p.column(p.z + step))

        last = ZS - 1
        for way, (step, at, todo) in enumerate(((1, distance, distance < zp), (-1, last - distance, last - distance > zp))):
            if todo:
                pl.when(p.z == at)(functools.partial(go, way, step))

    def final(self, zp):
        @pl.when(self.p.z == zp)
        def _():
            for k, part in enumerate(self.s.chunks):
                for way, end in enumerate((0, ZS - 1)):
                    if zp != end:
                        self.line_in(way, zp, k, part)

    def drain(self):
        p = self.p
        self.slab.drain()
        p.elsewhere(lambda zp: wait_for(self.slabs.at[zp], self.bsems[zp][0]))

        def sent(way, zp):
            for k, part in enumerate(self.s.chunks):
                wait_for(self.line.at[way, zp, part], self.zsems.under(way).under(zp)[k][0])

        for zp in range(ZS):
            wait_for(self.fromc.at[zp], self.csems[zp][0])
            self.planes[zp].drain()
            for way, cond in enumerate((p.z < zp, p.z > zp)):
                pl.when(cond)(functools.partial(sent, way, zp))

    def run(self, fill=lambda: None):
        one, two, three, four = Z_ORDER
        planes = self.planes
        for zp in Z_ORDER:
            self.begin(zp)
        for zp in Z_ORDER:
            self.both_cores(zp)
            if zp in (one, two):
                planes[zp].start()
            self.slab_out(zp)
        fill()
        planes[one].middle()
        planes[three].start()
        fill()
        planes[one].end()
        self.hop(one, 0)
        fill()
        planes[two].middle()
        planes[four].start()
        fill()
        planes[two].end()
        self.hop(two, 0)
        self.hop(one, 1)
        fill()
        planes[three].middle()
        fill()
        planes[three].end()
        self.hop(three, 0)
        self.hop(two, 1)
        self.hop(one, TWO)
        fill()
        self.p.elsewhere(self.slab_sum)
        self.slab.start()
        planes[four].middle()
        self.slab.middle()
        planes[four].end()
        self.hop(four, 0)
        self.hop(three, 1)
        self.hop(two, TWO)
        self.hop(four, 1)
        self.slab.end()
        for zp in Z_ORDER:
            self.final(zp)


class PlaneGather:
    def __init__(self, p, plane, colours, sems):
        one, two = colours
        mine, ynb, xnb, far = (plane.at[y, x, p.c] for y, x in ((p.y, p.x), (p.oy, p.x), (p.y, p.ox), (p.oy, p.ox)))
        self.mine, self.blocks, self.sems = mine, (ynb, xnb, far), sems
        self.moves = ((mine, one, p.yn), (mine, two, p.xn), (mine, two, p.yn), (mine, one, p.xn), (ynb, one, p.xn), (xnb, two, p.yn))

    def send(self, k, src=None):
        block, at, peer = self.moves[k]
        remote((block if src is None else src).at[at], block.at[at], self.sems[k], peer)

    def got(self, k, side=1):
        block, at, peer = self.moves[k]
        wait_for(block.at[at], self.sems[k][side])

    def start(self, src):
        for k in range(ZS):
            self.send(k, src)

    def relay(self):
        for k in range(TWO):
            self.got(k)
            self.send(k + ZS)

    def rest(self, forward=None):
        waits = ((TWO,), (3,), (ZS, 5))
        for ks, block in zip(waits, self.blocks):
            for k in ks:
                self.got(k)
            if forward is not None:
                forward(block)

    def drain(self):
        for k in range(len(self.moves)):
            self.got(k, 0)


class AllGather:
    scratch = [*Sems.scratch(TWO, ZS), *Sems.scratch(ZS, 6), *Sems.scratch(ZS), *Sems.scratch(ZS), *Sems.scratch(6), DMA]

    def __init__(self, p, own, out, s, scratch):
        self.p, self.own, self.out, self.s = p, own, out, s
        *pairs, self.lsem = scratch
        self.zsems, self.plane_sems, self.csems, self.bsems, slab_sems = (Sems(pair) for pair in zip(pairs[::TWO], pairs[1::TWO]))
        self.slab = PlaneGather(p, out.at[p.z], s.colours[1], slab_sems)

    def plane(self, zp):
        return PlaneGather(self.p, self.out.at[zp], self.s.colours[0], self.plane_sems.under(zp))

    def band(self, zp):
        return self.out.at[zp, :, :, self.p.c, self.s.all_b]

    def forward(self, zp, src, dst):
        remote(src, dst, self.csems[zp], self.p.core)

    def spread(self, zp, src):
        plane, a = self.plane(zp), self.s.all_a
        plane.start(src)
        self.forward(zp, src.at[a], plane.mine.at[a])

    def send_z(self, way, zp, src):
        p = self.p
        step, end = ((1, ZS - 1), (-1, 0))[way]

        @pl.when(p.z != end)
        def _():
            remote(src, self.plane(zp).mine.at[self.s.all_a], self.zsems.under(way)[zp], p.column(p.z + step))

    def arrive(self, way, zp):
        mine = self.plane(zp).mine
        part = mine.at[self.s.all_a]
        wait_for(part, self.zsems.under(way)[zp][1])
        self.send_z(way, zp, part)
        self.spread(zp, mine)

    def relay(self, way, zp):
        self.plane(zp).relay()

    def finish(self, way, zp):
        def forward(block):
            part = block.at[self.s.all_a]
            self.forward(zp, part, part)

        self.plane(zp).rest(forward)

    def at_distance(self, d, *fns):
        z = self.p.z
        for fn in fns:
            if d:
                pl.when(z >= d)(functools.partial(fn, 0, z - d))
                pl.when(z + d < ZS)(functools.partial(fn, 1, z + d))
            else:
                fn(0, z)

    def band_out(self):
        p, band = self.p, self.band(self.p.z)
        self.forward(p.z, band, band)
        p.elsewhere(lambda zp: remote(band, band, (self.bsems[zp][0], self.bsems[p.z][1]), p.column(zp)))

    def band_in(self, zp):
        band = self.band(zp)
        wait_for(band, self.bsems[zp][1])
        self.forward(zp, band, band)

    def run(self, fill=lambda: None):
        p = self.p
        local(self.own, self.slab.mine, self.lsem)
        self.slab.start(self.own)
        for way in range(TWO):
            self.send_z(way, p.z, self.own.at[self.s.all_a])
        self.spread(p.z, self.own)
        fill()
        self.slab.relay()
        wait_for(self.own, self.lsem)
        near, mid, far = range(1, ZS)
        self.at_distance(0, self.relay)
        fill()
        self.at_distance(near, self.arrive)
        fill()
        self.at_distance(mid, self.arrive)
        self.slab.rest()
        self.band_out()
        self.at_distance(0, self.finish)
        fill()
        self.at_distance(near, self.relay)
        self.at_distance(far, self.arrive)
        fill()
        self.at_distance(near, self.finish)
        self.at_distance(mid, self.relay, self.finish)
        self.at_distance(far, self.relay)
        p.elsewhere(self.band_in)
        self.at_distance(far, self.finish)
        self.slab.drain()
        p.elsewhere(lambda zp: wait_for(self.band(zp), self.bsems[zp][0]))
        part = self.slab.mine.at[self.s.all_a]

        def sent(way, zp):
            wait_for(part, self.zsems.under(way)[zp][0])

        for zp in range(ZS):
            for sem in self.csems[zp]:
                wait_for(self.out.at[zp, :, :, p.c], sem)
            self.plane(zp).drain()
            for way, cond in enumerate(((p.z < ZS - 1) & (p.z >= zp), (p.z > 0) & (p.z <= zp))):
                pl.when(cond)(functools.partial(sent, way, zp))


class Filler:
    def __init__(self, body, share):
        self.body, self.share, self.at = body, share, 0

    def __call__(self):
        stop = min(self.at + self.share, TILES)
        if self.at < stop:
            lax.fori_loop(self.at, stop, lambda i, carry: self.body(i) or carry, 0)
        self.at = stop

    def finish(self):
        while self.at < TILES:
            self()


def tile_at(i):
    return pl.ds(pl.multiple_of(i * TILE, 128), TILE)


def drain_tiles(buf, sems):
    for slot in range(TWO):
        wait_for(buf.at[slot], sems.at[slot])


def comm_params(ident):
    return pltpu.CompilerParams(collective_id=ident, has_side_effects=True, vmem_limit_bytes=VMEM_LIMIT)


def gather_kernel(split, own, d_mods, act, out, wgrad, mods, acc, load_sem, tile_sem, *scratch):
    local(d_mods, mods, load_sem)
    peers = Peers()
    peers.barrier()

    def tile(i):
        slot = lax.rem(i, TWO)

        @pl.when(i >= TWO)
        def _():
            wait_for(acc.at[slot], tile_sem.at[slot])

        @pl.when(i == 0)
        def _():
            wait_for(mods, load_sem)

        acc[slot] = lax.dot_general(mods[:, tile_at(i)], act[...], CONTRACT_ROWS, preferred_element_type=F32)
        local(acc.at[slot], wgrad.at[tile_at(i)], tile_sem.at[slot])

    fill = Filler(tile, 3)
    AllGather(peers, own, out, split, scratch).run(fill)
    fill.finish()
    drain_tiles(acc, tile_sem)


def gather_blocks(block, d_mods, act):
    split = Split(*WMOD_SPLIT)
    return pl.pallas_call(
        functools.partial(gather_kernel, split),
        out_shape=[jax.ShapeDtypeStruct((ZS, TWO, TWO, TWO, split.rows, WIDTH), block.dtype), jax.ShapeDtypeStruct((MOD, WIDTH), F32)],
        in_specs=[ANY, ANY, IN_VMEM], out_specs=[ANY, ANY],
        scratch_shapes=[pltpu.VMEM(d_mods.shape, BF16), pltpu.VMEM((TWO, TILE, WIDTH), F32), DMA, DMA((TWO,)), *AllGather.scratch],
        compiler_params=comm_params(0), name="gather_wmod",
    )(block, d_mods, act)


def scatter_kernel(pieces, split, source, out, sem, *scratch):
    peers = Peers()
    peers.barrier()
    rs = ReduceScatter(peers, [source], pieces, split, scratch)
    rs.run()
    local(rs.part.at[peers.z, peers.y, peers.x], out, sem)
    rs.drain()
    wait_for(out, sem)


def scatter_sum(partial, pieces):
    split = Split(*WGRAD_SPLIT)
    return pl.pallas_call(
        functools.partial(scatter_kernel, pieces, split),
        out_shape=jax.ShapeDtypeStruct((split.rows, WIDTH), F32),
        in_specs=[ANY], out_specs=ANY, scratch_shapes=[DMA] + ReduceScatter.scratch(split),
        compiler_params=comm_params(1), name="scatter_wgrad",
    )(partial)


def reduce_kernel(pieces, split, count, *refs):
    sources, (act, weight, bias, out, mods, tiles, acc, load_sem, tile_sem), scratch = refs[:count], refs[count:count + 9], refs[count + 9:]
    peers = Peers()
    peers.barrier()

    def load(i):
        slot = lax.rem(i, TWO)
        local(weight.at[tile_at(i)], tiles.at[slot], load_sem.at[slot])

    def tile(i):
        slot = lax.rem(i, TWO)

        @pl.when(i >= TWO)
        def _():
            wait_for(acc.at[slot], tile_sem.at[slot])

        @pl.when(i < TILES - 1)
        def _():
            load(i + 1)

        wait_for(tiles.at[slot], load_sem.at[slot])
        product = lax.dot_general(act[...], tiles[slot], CONTRACT_COLS, preferred_element_type=F32)
        acc[slot] = (product + bias[:, tile_at(i)]).astype(BF16)
        local(acc.at[slot], mods.at[:, tile_at(i)], tile_sem.at[slot])

    load(0)
    fill = Filler(tile, 3)
    own = len(AllGather.scratch)
    rs = ReduceScatter(peers, sources, pieces, split, scratch[own:])
    rs.run(fill)
    fill.finish()
    AllGather(peers, rs.part.at[peers.z, peers.y, peers.x], out, split, scratch[:own]).run()
    rs.drain()
    drain_tiles(acc, tile_sem)


def reduce_all(sources, pieces, act, weight, bias):
    split = Split(*EMBED_SPLIT)
    return pl.pallas_call(
        functools.partial(reduce_kernel, pieces, split, len(sources)),
        out_shape=[jax.ShapeDtypeStruct((ZS, TWO, TWO, TWO, split.rows, WIDTH), F32), jax.ShapeDtypeStruct((ROWS, MOD), BF16)],
        in_specs=[ANY] * len(sources) + [IN_VMEM, ANY, IN_VMEM], out_specs=[ANY, ANY],
        scratch_shapes=[pltpu.VMEM((TWO, TILE, WIDTH), BF16), pltpu.VMEM((TWO, ROWS, TILE), BF16), DMA((TWO,)), DMA((TWO,)), *AllGather.scratch] + ReduceScatter.scratch(split),
        compiler_params=comm_params(TWO), name="reduce_embed",
    )(*sources, act, weight, bias)


def unpack_kernel(pieces, total, *refs):
    *outs, buf, load_sem, store_sem = refs
    order = [(zp, core) for zp in range(ZS) for core in range(TWO)]
    for at in order:
        local(total.at[at[0], :, :, at[1]], buf.at[at], load_sem.at[at])
    for at in order:
        wait_for(buf.at[at], load_sem.at[at])
        zp, core = at
        for dst, start, n, row in pieces[core]:
            local(buf.at[zp, core, :, :, pl.ds(row, n)], outs[dst].at[zp, :, :, pl.ds(start, n)], store_sem.at[at])
    for at in order:
        wait_for(buf.at[at], store_sem.at[at])


def unpack(total, sources, pieces):
    return pl.pallas_call(
        functools.partial(unpack_kernel, pieces),
        out_shape=[jax.ShapeDtypeStruct(s.shape, s.dtype) for s in sources],
        in_specs=[ANY], out_specs=[ANY] * len(sources),
        scratch_shapes=[pltpu.VMEM((ZS, TWO, TWO, TWO, *total.shape[ZS:]), F32), DMA((ZS, TWO)), DMA((ZS, TWO))],
        compiler_params=pltpu.CompilerParams(vmem_limit_bytes=VMEM_LIMIT), name="unpack",
    )(total)


def outer_kernel(left, right, out):
    out[...] = lax.dot_general(left[...], right[...], CONTRACT_ROWS, preferred_element_type=F32)


def outer(left, right):
    rows, n = left.shape
    return pl.pallas_call(
        outer_kernel,
        grid=(n // rows,),
        out_shape=jax.ShapeDtypeStruct((n, WIDTH), F32),
        in_specs=[pl.BlockSpec((rows, rows), lambda i: (0, i)), pl.BlockSpec((rows, WIDTH), lambda i: (0, 0))],
        out_specs=pl.BlockSpec((rows, WIDTH), lambda i: (i, 0)),
        compiler_params=pltpu.CompilerParams(vmem_limit_bytes=VMEM_LIMIT), name="outer",
    )(left, right)


def sinusoid(values, freq_width):
    half_width = freq_width // 2
    freq_table = jnp.exp(-math.log(MAX_PERIOD) * jnp.arange(half_width, dtype=F32) / half_width)
    angles = (TIME_SCALE * values)[:, None] * freq_table[None, :]
    return jnp.concatenate([jnp.cos(angles), jnp.sin(angles)], axis=1).astype(BF16)


def silu_grad(values):
    sigmoid_v = jax.nn.sigmoid(values)
    return sigmoid_v * (1.0 + values * (1.0 - sigmoid_v))


def mlp_forward(inputs_bf, params):
    hidden = jnp.dot(inputs_bf, params[0], preferred_element_type=F32) + params[1].astype(F32)
    act_bf = jax.nn.silu(hidden).astype(BF16)
    output = jnp.dot(act_bf, params[2], preferred_element_type=F32) + params[3].astype(F32)
    return output, hidden, act_bf


def mlp_backward(inputs_bf, params, hidden, act_bf, d_out_bf):
    grad_w2 = lax.dot_general(act_bf, d_out_bf, CONTRACT_ROWS, preferred_element_type=F32)
    d_act = lax.dot_general(d_out_bf, params[2], CONTRACT_COLS, preferred_element_type=F32)
    d_hidden = d_act * silu_grad(hidden)
    d_hidden_bf = d_hidden.astype(BF16)
    if inputs_bf.shape[1] > d_hidden_bf.shape[1]:
        grad_w1 = outer(inputs_bf, d_hidden_bf)
    else:
        grad_w1 = lax.dot_general(inputs_bf, d_hidden_bf, CONTRACT_ROWS, preferred_element_type=F32)
    grad_b1 = jnp.sum(d_hidden, axis=0)
    return grad_w1, grad_b1, grad_w2


def by_chip(grad):
    return grad.reshape(ZS, TWO, TWO, grad.shape[0] // CHIPS, WIDTH)


WGRAD_PIECES = (((0, 0, 184, 0),), ((0, 176, 184, 0),))
EMBED_PIECES = (
    ((0, 0, 16, 0), (1, 0, 16, 16), (2, 0, 128, 32), (6, 0, 8, 160), (3, 0, 24, 168)),
    ((3, 24, 48, 0), (4, 0, 72, 48), (5, 0, 72, 120)),
)


def solution(mesh):
    row_split = P(AXIS)
    row_matrix = P(AXIS, None)
    col_matrix = P(None, AXIS)
    embed_specs = (P(None, None), P(None), P(None, None), P(None)) * 3
    in_specs = (row_split, row_split, row_matrix) + embed_specs + (col_matrix, row_split, row_matrix)
    out_specs = (row_matrix, col_matrix, row_split) + embed_specs

    def local_step(timesteps, guidance, pooled, time_w1, time_b1, time_w2, time_b2, guide_w1, guide_b1, guide_w2, guide_b2, text_w1, text_b1, text_w2, text_b2, w_mod, b_mod, d_mods):
        me = lax.axis_index(AXIS)
        freq_width = time_w1.shape[0]
        inputs_list = [sinusoid(timesteps, freq_width), sinusoid(guidance, freq_width), pooled]
        params_list = [(time_w1, time_b1, time_w2, time_b2), (guide_w1, guide_b1, guide_w2, guide_b2), (text_w1, text_b1, text_w2, text_b2)]
        saved = [mlp_forward(u, params) for u, params in zip(inputs_list, params_list)]
        cond_vec = saved[0][0] + saved[1][0] + saved[2][0]
        cond_silu = jax.nn.silu(cond_vec).astype(BF16)

        extra = jnp.pad(b_mod[None, :], ((0, PADDED - SHARE - 1), (0, WIDTH - SHARE)))
        gathered, part_wgrad = gather_blocks(jnp.concatenate([w_mod.T, extra], axis=0), d_mods, cond_silu)
        gathered = gathered.reshape(DEVICES, PADDED, WIDTH)
        full_wt = gathered[:, :SHARE].reshape(MOD, WIDTH)
        full_b = gathered[:, SHARE, :SHARE].reshape(1, MOD).astype(F32)
        wgrad = scatter_sum(by_chip(part_wgrad), WGRAD_PIECES)
        grad_wmod = lax.dynamic_slice(wgrad, (4 * lax.rem(me, TWO), 0), (SHARE, WIDTH)).T

        d_cond = jnp.dot(d_mods, full_wt, preferred_element_type=F32)
        d_vec = d_cond * silu_grad(cond_vec)
        d_vec_bf = d_vec.astype(BF16)
        grads = [mlp_backward(u, params, record[1], record[2], d_vec_bf) for u, params, record in zip(inputs_list, params_list, saved)]
        bgrad_rows = MOD // WIDTH
        part_bgrad = jnp.sum(d_mods, axis=0, dtype=F32).reshape(bgrad_rows, WIDTH)
        vectors = [g[1] for g in grads] + [jnp.sum(d_vec, axis=0)]
        vectors = jnp.concatenate([jnp.stack(vectors), part_bgrad], axis=0)
        vectors = jnp.pad(vectors, ((0, 128 - vectors.shape[0]), (0, 0)))
        sources = [by_chip(g) for g in [g[0] for g in grads] + [g[2] for g in grads] + [vectors]]
        total, modulation = reduce_all(sources, EMBED_PIECES, cond_silu, full_wt, full_b)
        *full, sums = [g.reshape(-1, WIDTH) for g in unpack(total, sources, EMBED_PIECES)]
        count = len(grads)
        grad_bmod = lax.dynamic_slice(sums[ZS:ZS + bgrad_rows].reshape(MOD), (SHARE * me,), (SHARE,))
        embed_grads = [g for i in range(count) for g in (full[i], sums[i], full[i + count], sums[count])]
        return (modulation, grad_wmod, grad_bmod, *embed_grads)

    return jax.shard_map(local_step, mesh=mesh, in_specs=in_specs, out_specs=out_specs, check_vma=False)
```

```python
import functools
import math
import jax
import jax.numpy as jnp
from jax import lax
from jax.experimental import pallas as pl
from jax.experimental.pallas import tpu as pltpu
from jax.sharding import PartitionSpec as P

AXIS = "fsdp"
MESH = pl.DeviceIdType.MESH
MAX_PERIOD = 10000.0
TIME_SCALE = 1000.0
CONTRACT_ROWS = (((0,), (0,)), ((), ()))
CONTRACT_COLS = (((1,), (1,)), ((), ()))
F32, BF16 = jnp.float32, jnp.bfloat16
VMEM_LIMIT = 62 << 20
TWO, ZS, CHIPS, DEVICES = 2, 4, 16, 32
ROWS, WIDTH, MOD, SHARE, PADDED = 512, 1152, 5760, 180, 184
TILE, TILES = 384, 15
Z_ORDER = (3, 0, 2, 1)
ANY = pl.BlockSpec(memory_space=pl.ANY)
IN_VMEM = pl.BlockSpec(memory_space=pltpu.VMEM)
DMA = pltpu.SemaphoreType.DMA
WMOD_SPLIT = (80, 64, 16, 24)
WGRAD_SPLIT = (72, 72, 24, 16)
EMBED_SPLIT = (80, 72, 24, 16)


class Peers:
    def __init__(self):
        me = lax.axis_index(AXIS)
        bits = []
        for _ in range(3):
            bits.append(lax.rem(me, TWO))
            me = lax.div(me, TWO)
        self.c, self.x, self.y = bits
        self.oc, self.ox, self.oy = (1 - bit for bit in bits)
        self.z = me
        self.core = self.device(me, self.y, self.x, self.oc)
        self.xn = self.device(me, self.y, self.ox, self.c)
        self.yn = self.device(me, self.oy, self.x, self.c)

    def device(self, z, y, x, c):
        return (((z * TWO + y) * TWO + x) * TWO + c,)

    def column(self, zp):
        return self.device(zp, self.y, self.x, self.c)

    def elsewhere(self, fn):
        for zp in range(ZS):
            pl.when(self.z != zp)(functools.partial(fn, zp))

    def barrier(self):
        sem = pltpu.get_barrier_semaphore()

        def greet(peer):
            pl.semaphore_signal(sem, device_id=peer, device_id_type=MESH)

        for peer in (self.core, self.xn, self.yn):
            greet(peer)
        self.elsewhere(lambda zp: greet(self.column(zp)))
        pl.semaphore_wait(sem, 6)


def remote(src, dst, sems, peer):
    pltpu.make_async_remote_copy(src_ref=src, dst_ref=dst, send_sem=sems[0], recv_sem=sems[1], device_id=peer, device_id_type=MESH).start()


def local(src, dst, sem):
    pltpu.make_async_copy(src, dst, sem).start()


def wait_for(ref, sem):
    pltpu.make_async_copy(ref, ref, sem).wait()


def add_rows(dst, src):
    if len(dst.shape) > TWO:
        for i in range(dst.shape[0]):
            add_rows(dst.at[i], src.at[i])
        return
    rows = dst.shape[0]
    step = 24 if rows % 24 == 0 else 8

    def body(i, carry):
        at = pl.ds(pl.multiple_of(i * step, 8), step)
        dst[at, :] = dst[at, :] + src[at, :]
        return carry

    lax.fori_loop(0, rows // step, body, 0)


class Sems:
    def __init__(self, refs, *index):
        self.send, self.recv, self.index = *refs, index

    def __getitem__(self, k):
        return self.send.at[(*self.index, k)], self.recv.at[(*self.index, k)]

    def under(self, k):
        return Sems((self.send, self.recv), *self.index, k)

    @staticmethod
    def scratch(*shape):
        return [DMA(shape), DMA(shape)]


class Split:
    def __init__(self, *n):
        starts = [sum(n[:i]) for i in range(ZS)]
        ranges = [pl.ds(start, size) for start, size in zip(starts, n)]
        self.n, self.colours = (n[:TWO], n[TWO:]), (ranges[:TWO], ranges[TWO:])
        self.a, self.b = sum(self.n[0]), sum(self.n[1])
        self.rows = self.a + self.b
        self.all_a, self.all_b = pl.ds(0, self.a), pl.ds(self.a, self.b)
        size = -(-self.a // DEVICES) * 8
        self.chunks = [pl.ds(at, min(size, self.a - at)) for at in range(0, self.a, size)]


class PlaneReduce:
    @staticmethod
    def shapes(sizes):
        one, two = sizes
        return [(TWO, one), (TWO, two), (one,), (two,)]

    def __init__(self, p, plane, colours, boxes, sems):
        one, two = colours
        x1, y1, y2, x2 = boxes
        self.sems = sems
        self.moves = (
            (plane.at[:, p.ox, one], x1, p.xn), (plane.at[p.oy, :, two], y1, p.yn),
            (plane.at[p.oy, p.x, one], y2, p.yn), (plane.at[p.y, p.ox, two], x2, p.xn),
        )
        mine = plane.at[p.y, p.x]
        self.first = ((x1.at[p.oy], x1.at[p.y]), (y1.at[p.ox], y1.at[p.x]))
        self.mine = (mine.at[one], mine.at[two])

    def send(self, k):
        src, dst, peer = self.moves[k]
        remote(src, dst, self.sems[k], peer)

    def got(self, k):
        wait_for(self.moves[k][1], self.sems[k][1])

    def start(self):
        for k in range(TWO):
            self.send(k)

    def middle(self):
        for k in range(TWO):
            self.got(k)
            add_rows(self.moves[k + TWO][0], self.first[k][0])
            self.send(k + TWO)
        for k in range(TWO):
            add_rows(self.mine[k], self.first[k][1])

    def end(self):
        for k in range(TWO):
            self.got(k + TWO)
            add_rows(self.mine[k], self.moves[k + TWO][1])

    def drain(self):
        for k, move in enumerate(self.moves):
            wait_for(move[1], self.sems[k][0])


class ReduceScatter:
    @staticmethod
    def scratch(s):
        whole = [(n, TWO, TWO, s.rows) for n in (ZS, TWO)]
        planes = [(ZS,) + shape for shape in PlaneReduce.shapes(s.n[0])] + PlaneReduce.shapes(s.n[1])
        shapes = whole + planes + [(TWO, ZS, s.a), (ZS, TWO, TWO, s.b)]
        buffers = [pltpu.VMEM(shape + (WIDTH,), F32) for shape in shapes]
        return buffers + [DMA((ZS,))] + Sems.scratch(ZS) + Sems.scratch(ZS, ZS) + Sems.scratch(TWO, ZS, len(s.chunks)) + Sems.scratch(ZS) + Sems.scratch(ZS)

    def __init__(self, p, sources, pieces, s, scratch):
        self.p, self.sources, self.pieces, self.s = p, sources, pieces, s
        scratch = list(scratch)
        take = lambda n: [scratch.pop(0) for _ in range(n)]
        self.part, self.own = take(TWO)
        boxes, slab_boxes = take(ZS), take(ZS)
        self.line, self.slabs, self.lsem = take(3)
        self.csems, plane_sems, self.zsems, self.bsems, slab_sems = (Sems(take(TWO)) for _ in range(5))
        self.planes = [PlaneReduce(p, self.part.at[zp], s.colours[0], [box.at[zp] for box in boxes], plane_sems.under(zp)) for zp in range(ZS)]
        self.slab = PlaneReduce(p, self.part.at[p.z], s.colours[1], slab_boxes, slab_sems)

    def partner(self, zp):
        def send(core):
            for src, start, n, at in self.pieces[1 - core]:
                remote(self.sources[src].at[zp, :, :, pl.ds(start, n)], self.part.at[zp, :, :, pl.ds(at, n)], self.csems[zp], self.p.core)

        self.by_core(send)

    def load(self, zp):
        slot = Z_ORDER.index(zp) % TWO

        def start(core):
            for src, at_src, n, at in self.pieces[core]:
                local(self.sources[src].at[zp, :, :, pl.ds(at_src, n)], self.own.at[slot, :, :, pl.ds(at, n)], self.lsem.at[zp])

        self.by_core(start)

    def by_core(self, fn):
        for core in range(TWO):
            pl.when(self.p.c == core)(functools.partial(fn, core))

    def both_cores(self, zp):
        own = self.own.at[Z_ORDER.index(zp) % TWO]
        wait_for(own, self.lsem.at[zp])
        wait_for(self.part.at[zp], self.csems[zp][1])
        add_rows(self.part.at[zp], own)

    def slab_out(self, zp):
        p = self.p

        @pl.when(p.z != zp)
        def _():
            sems = self.bsems[zp][0], self.bsems[p.z][1]
            remote(self.part.at[zp, :, :, self.s.all_b], self.slabs.at[p.z], sems, p.column(zp))

    def slab_sum(self, zp):
        wait_for(self.slabs.at[zp], self.bsems[zp][1])
        add_rows(self.part.at[self.p.z, :, :, self.s.all_b], self.slabs.at[zp])

    def line_in(self, way, zp, k, part):
        box = self.line.at[way, zp, part]
        wait_for(box, self.zsems.under(way).under(zp)[k][1])
        add_rows(self.part.at[zp, self.p.y, self.p.x, part], box)

    def hop(self, zp, distance):
        p = self.p

        def go(way, step):
            for k, part in enumerate(self.s.chunks):
                if distance:
                    self.line_in(way, zp, k, part)
                remote(self.part.at[zp, p.y, p.x, part], self.line.at[way, zp, part], self.zsems.under(way).under(zp)[k], p.column(p.z + step))

        last = ZS - 1
        for way, (step, at, todo) in enumerate(((1, distance, distance < zp), (-1, last - distance, last - distance > zp))):
            if todo:
                pl.when(p.z == at)(functools.partial(go, way, step))

    def final(self, zp):
        @pl.when(self.p.z == zp)
        def _():
            for k, part in enumerate(self.s.chunks):
                for way, end in enumerate((0, ZS - 1)):
                    if zp != end:
                        self.line_in(way, zp, k, part)

    def drain(self):
        p = self.p
        self.slab.drain()
        p.elsewhere(lambda zp: wait_for(self.slabs.at[zp], self.bsems[zp][0]))

        def sent(way, zp):
            for k, part in enumerate(self.s.chunks):
                wait_for(self.line.at[way, zp, part], self.zsems.under(way).under(zp)[k][0])

        for zp in range(ZS):
            wait_for(self.part.at[zp], self.csems[zp][0])
            self.planes[zp].drain()
            for way, cond in enumerate((p.z < zp, p.z > zp)):
                pl.when(cond)(functools.partial(sent, way, zp))

    def run(self, fill=lambda: None):
        one, two, three, four = Z_ORDER
        planes = self.planes
        for zp in Z_ORDER:
            self.partner(zp)
        self.load(one)
        self.load(two)
        fill()
        for zp, later in zip(Z_ORDER, (three, four, None, None)):
            self.both_cores(zp)
            if later is None:
                self.slab_out(zp)
            else:
                self.load(later)
                planes[zp].start()
                self.slab_out(zp)
            fill()
        planes[one].middle()
        planes[three].start()
        fill()
        planes[one].end()
        self.hop(one, 0)
        fill()
        planes[two].middle()
        planes[four].start()
        fill()
        planes[two].end()
        self.hop(two, 0)
        self.hop(one, 1)
        fill()
        planes[three].middle()
        fill()
        planes[three].end()
        self.hop(three, 0)
        self.hop(two, 1)
        self.hop(one, TWO)
        fill()
        self.p.elsewhere(self.slab_sum)
        self.slab.start()
        fill()
        planes[four].middle()
        self.slab.middle()
        fill()
        planes[four].end()
        self.hop(four, 0)
        self.hop(three, 1)
        self.hop(two, TWO)
        self.hop(four, 1)
        self.slab.end()
        fill()
        for zp in Z_ORDER:
            self.final(zp)


class PlaneGather:
    def __init__(self, p, plane, colours, sems):
        one, two = colours
        mine, ynb, xnb, far = (plane.at[y, x, p.c] for y, x in ((p.y, p.x), (p.oy, p.x), (p.y, p.ox), (p.oy, p.ox)))
        self.mine, self.blocks, self.sems = mine, (ynb, xnb, far), sems
        self.moves = ((mine, one, p.yn), (mine, two, p.xn), (mine, two, p.yn), (mine, one, p.xn), (ynb, one, p.xn), (xnb, two, p.yn))

    def send(self, k, src=None):
        block, at, peer = self.moves[k]
        remote((block if src is None else src).at[at], block.at[at], self.sems[k], peer)

    def got(self, k, side=1):
        block, at, peer = self.moves[k]
        wait_for(block.at[at], self.sems[k][side])

    def start(self, src):
        for k in range(ZS):
            self.send(k, src)

    def relay(self):
        for k in range(TWO):
            self.got(k)
            self.send(k + ZS)

    def rest(self, forward=None):
        waits = ((TWO,), (3,), (ZS, 5))
        for ks, block in zip(waits, self.blocks):
            for k in ks:
                self.got(k)
            if forward is not None:
                forward(block)

    def drain(self):
        for k in range(len(self.moves)):
            self.got(k, 0)


class AllGather:
    scratch = [*Sems.scratch(TWO, ZS), *Sems.scratch(ZS, 6), *Sems.scratch(ZS), *Sems.scratch(ZS), *Sems.scratch(6), DMA]

    def __init__(self, p, own, out, s, scratch):
        self.p, self.own, self.out, self.s = p, own, out, s
        *pairs, self.lsem = scratch
        self.zsems, self.plane_sems, self.csems, self.bsems, slab_sems = (Sems(pair) for pair in zip(pairs[::TWO], pairs[1::TWO]))
        self.slab = PlaneGather(p, out.at[p.z], s.colours[1], slab_sems)

    def plane(self, zp):
        return PlaneGather(self.p, self.out.at[zp], self.s.colours[0], self.plane_sems.under(zp))

    def band(self, zp):
        return self.out.at[zp, :, :, self.p.c, self.s.all_b]

    def forward(self, zp, src, dst):
        remote(src, dst, self.csems[zp], self.p.core)

    def spread(self, zp, src):
        plane, a = self.plane(zp), self.s.all_a
        plane.start(src)
        self.forward(zp, src.at[a], plane.mine.at[a])

    def send_z(self, way, zp, src):
        p = self.p
        step, end = ((1, ZS - 1), (-1, 0))[way]

        @pl.when(p.z != end)
        def _():
            remote(src, self.plane(zp).mine.at[self.s.all_a], self.zsems.under(way)[zp], p.column(p.z + step))

    def arrive(self, way, zp):
        mine = self.plane(zp).mine
        part = mine.at[self.s.all_a]
        wait_for(part, self.zsems.under(way)[zp][1])
        self.send_z(way, zp, part)
        self.spread(zp, mine)

    def relay(self, way, zp):
        self.plane(zp).relay()

    def finish(self, way, zp):
        def forward(block):
            part = block.at[self.s.all_a]
            self.forward(zp, part, part)

        self.plane(zp).rest(forward)

    def at_distance(self, d, *fns):
        z = self.p.z
        for fn in fns:
            if d:
                pl.when(z >= d)(functools.partial(fn, 0, z - d))
                pl.when(z + d < ZS)(functools.partial(fn, 1, z + d))
            else:
                fn(0, z)

    def band_out(self):
        p, band = self.p, self.band(self.p.z)
        self.forward(p.z, band, band)
        p.elsewhere(lambda zp: remote(band, band, (self.bsems[zp][0], self.bsems[p.z][1]), p.column(zp)))

    def band_in(self, zp):
        band = self.band(zp)
        wait_for(band, self.bsems[zp][1])
        self.forward(zp, band, band)

    def run(self, fill=lambda: None):
        p = self.p
        local(self.own, self.slab.mine, self.lsem)
        self.slab.start(self.own)
        for way in range(TWO):
            self.send_z(way, p.z, self.own.at[self.s.all_a])
        self.spread(p.z, self.own)
        fill()
        self.slab.relay()
        wait_for(self.own, self.lsem)
        near, mid, far = range(1, ZS)
        self.at_distance(0, self.relay)
        fill()
        self.at_distance(near, self.arrive)
        fill()
        self.at_distance(mid, self.arrive)
        self.slab.rest()
        self.band_out()
        self.at_distance(0, self.finish)
        fill()
        self.at_distance(near, self.relay)
        self.at_distance(far, self.arrive)
        fill()
        self.at_distance(near, self.finish)
        self.at_distance(mid, self.relay, self.finish)
        self.at_distance(far, self.relay)
        p.elsewhere(self.band_in)
        self.at_distance(far, self.finish)
        self.slab.drain()
        p.elsewhere(lambda zp: wait_for(self.band(zp), self.bsems[zp][0]))
        part = self.slab.mine.at[self.s.all_a]

        def sent(way, zp):
            wait_for(part, self.zsems.under(way)[zp][0])

        for zp in range(ZS):
            for sem in self.csems[zp]:
                wait_for(self.out.at[zp, :, :, p.c], sem)
            self.plane(zp).drain()
            for way, cond in enumerate(((p.z < ZS - 1) & (p.z >= zp), (p.z > 0) & (p.z <= zp))):
                pl.when(cond)(functools.partial(sent, way, zp))


class Job:
    def __init__(self, count, body, load=None):
        self.count, self.body, self.load = count, body, load


class Filler:
    def __init__(self, jobs, share):
        self.jobs, self.share, self.job, self.at = jobs, share, 0, 0

    def prime(self):
        self.jobs[0].load(0)

    def part(self, stop):
        job, last = self.jobs[self.job], self.jobs[self.job].count - 1
        after = next((j.load for j in self.jobs[self.job + 1:] if j.load), None)

        def tile(i, carry):
            if job.load:
                @pl.when(i < last)
                def _():
                    job.load(i + 1)

                if after:
                    pl.when(i == last)(lambda: after(0))
            job.body(i)
            return carry

        lax.fori_loop(self.at, stop, tile, 0)

    def __call__(self):
        left = self.share
        while left and self.job < len(self.jobs):
            count = self.jobs[self.job].count
            stop = min(self.at + left, count)
            self.part(stop)
            left -= stop - self.at
            self.at = stop
            if stop == count:
                self.job, self.at = self.job + 1, 0

    def finish(self):
        while self.job < len(self.jobs):
            self()


class Stream:
    def __init__(self, buf, sems, base=0):
        self.buf, self.sems, self.base = buf, sems, base

    def slot(self, i):
        return lax.rem(i + self.base, TWO)

    def load(self, i, src):
        slot = self.slot(i)
        local(src, self.buf.at[slot], self.sems.at[slot])

    def ready(self, i):
        slot = self.slot(i)
        wait_for(self.buf.at[slot], self.sems.at[slot])
        return self.buf[slot]

    def store(self, i, value, dst):
        slot = self.slot(i)

        @pl.when(i + self.base >= TWO)
        def _():
            wait_for(self.buf.at[slot], self.sems.at[slot])

        self.buf[slot] = value
        local(self.buf.at[slot], dst, self.sems.at[slot])

    def drain(self):
        for slot in range(TWO):
            wait_for(self.buf.at[slot], self.sems.at[slot])

    def after(self, count):
        return Stream(self.buf, self.sems, self.base + count)

    @staticmethod
    def scratch(dtype, *shape):
        return [pltpu.VMEM((TWO, *shape), dtype), DMA((TWO,))]


def tile_at(i, width=TILE, start=0):
    return pl.ds(pl.multiple_of(start + i * width, 128), width)


def dot_rows(left, right):
    return lax.dot_general(left, right, CONTRACT_ROWS, preferred_element_type=F32)


def dot_cols(left, right):
    return lax.dot_general(left, right, CONTRACT_COLS, preferred_element_type=F32)


def comm_params(ident):
    return pltpu.CompilerParams(collective_id=ident, has_side_effects=True, vmem_limit_bytes=VMEM_LIMIT)


def gather_kernel(split, own, d_mods, act, out, wgrad, mods, load_sem, *scratch):
    local(d_mods, mods, load_sem)
    peers = Peers()
    peers.barrier()
    tiles, scratch = Stream(*scratch[:TWO]), scratch[TWO:]

    def tile(i):
        @pl.when(i == 0)
        def _():
            wait_for(mods, load_sem)

        tiles.store(i, dot_rows(mods[:, tile_at(i)], act[...]), wgrad.at[tile_at(i)])

    fill = Filler([Job(TILES, tile)], TWO)
    AllGather(peers, own, out, split, scratch).run(fill)
    fill.finish()
    tiles.drain()


def gather_blocks(block, d_mods, act):
    split = Split(*WMOD_SPLIT)
    return pl.pallas_call(
        functools.partial(gather_kernel, split),
        out_shape=[jax.ShapeDtypeStruct((ZS, TWO, TWO, TWO, split.rows, WIDTH), block.dtype), jax.ShapeDtypeStruct((MOD, WIDTH), F32)],
        in_specs=[ANY, ANY, IN_VMEM], out_specs=[ANY, ANY],
        scratch_shapes=[pltpu.VMEM(d_mods.shape, BF16), DMA, *Stream.scratch(F32, TILE, WIDTH), *AllGather.scratch],
        compiler_params=comm_params(0), name="gather_wmod",
    )(block, d_mods, act)


def scatter_kernel(pieces, split, mlps, *refs):
    refs = list(refs)
    take = lambda n: [refs.pop(0) for _ in range(n)]
    source, d_mods, weight, cond = take(ZS)
    hidden, second, inputs, acts = (take(mlps) for _ in range(ZS))
    out, sums = take(TWO)
    grads1, grads2 = take(mlps), take(mlps)
    mods, dcond, cvec, sem, mods_sem, cond_sem = take(6)
    wtiles, htiles, ltiles, stiles, lsmall, ssmall = (Stream(*take(TWO)) for _ in range(6))
    small = lsmall.buf.shape[-1]
    local(d_mods, mods, mods_sem)
    local(cond, cvec, cond_sem)
    peers = Peers()
    peers.barrier()
    rs = ReduceScatter(peers, [source], pieces, split, refs)

    def vector(k):
        return mods.at[:, pl.ds(k * WIDTH, WIDTH)]

    def d_cond(i):
        @pl.when(i == 0)
        def _():
            wait_for(mods, mods_sem)

        product = jnp.dot(mods[:, tile_at(i)], wtiles.ready(i), preferred_element_type=F32)
        dcond[...] = jnp.where(i == 0, 0.0, dcond[...]) + product

    def d_vec(i):
        @pl.when(i == 0)
        def _():
            wait_for(cvec, cond_sem)
            sums[...] = jnp.zeros_like(sums)

        at = tile_at(i, small)
        value = dcond[at, :] * silu_grad(cvec[at, :])
        mods[at, :WIDTH] = value.astype(BF16)
        sums[mlps:mlps + 1, :] += jnp.sum(value, axis=0, keepdims=True)

    per = WIDTH // TILE
    jobs = [Job(TILES, d_cond, lambda i: wtiles.load(i, weight.at[tile_at(i)])), Job(ROWS // small, d_vec)]
    for k in range(mlps):
        w, h = wtiles.after(TILES + k * per), htiles.after(k * per)

        def load(i, k=k, w=w, h=h):
            w.load(i, second[k].at[tile_at(i)])
            h.load(i, hidden[k].at[:, tile_at(i)])

        def d_hidden(i, k=k, w=w, h=h):
            value = dot_cols(vector(0)[...], w.ready(i)) * silu_grad(h.ready(i))
            mods[:, tile_at(i, start=(k + 1) * WIDTH)] = value.astype(BF16)
            sums[k:k + 1, tile_at(i)] = jnp.sum(value, axis=0, keepdims=True)

        jobs.append(Job(per, d_hidden, load))

    def outer(count, left, right, dst, lefts, stages, width):
        def load(i):
            lefts.load(i, left.at[:, tile_at(i, width)])

        def body(i):
            stages.store(i, dot_rows(lefts.ready(i), right[...]), dst.at[tile_at(i, width)])

        jobs.append(Job(count, body, load))

    done = 0
    for k in range(mlps):
        outer(per, acts[k], vector(0), grads2[k], ltiles.after(k * per), stiles.after(k * per), TILE)
    for k in range(mlps):
        count = inputs[k].shape[1] // small
        outer(count, inputs[k], vector(k + 1), grads1[k], lsmall.after(done), ssmall.after(done), small)
        done += count
    fill = Filler(jobs, ZS)
    fill.prime()
    rs.run(fill)
    local(rs.part.at[peers.z, peers.y, peers.x], out, sem)
    fill.finish()
    stiles.drain()
    ssmall.drain()
    rs.drain()
    wait_for(out, sem)


def scatter_sum(partial, d_mods, weight, cond, hidden, second, inputs, acts, pieces):
    split = Split(*WGRAD_SPLIT)
    args = [partial, d_mods, weight, cond, *hidden, *second, *inputs, *acts]
    small = inputs[0].shape[1]
    grads = [jax.ShapeDtypeStruct((a.shape[1], WIDTH), F32) for a in (*inputs, *acts)]
    return pl.pallas_call(
        functools.partial(scatter_kernel, pieces, split, len(hidden)),
        out_shape=[jax.ShapeDtypeStruct((split.rows, WIDTH), F32), jax.ShapeDtypeStruct((8, WIDTH), F32), *grads],
        in_specs=[ANY] * len(args), out_specs=[ANY, IN_VMEM] + [ANY] * len(grads),
        scratch_shapes=[
            pltpu.VMEM(d_mods.shape, BF16), pltpu.VMEM(cond.shape, F32), pltpu.VMEM(cond.shape, F32), DMA, DMA, DMA,
            *Stream.scratch(BF16, TILE, WIDTH), *Stream.scratch(F32, ROWS, TILE), *Stream.scratch(BF16, ROWS, TILE), *Stream.scratch(F32, TILE, WIDTH),
            *Stream.scratch(BF16, ROWS, small), *Stream.scratch(F32, small, WIDTH), *ReduceScatter.scratch(split),
        ],
        compiler_params=comm_params(1), name="scatter_wgrad",
    )(*args)


def reduce_kernel(pieces, split, count, *refs):
    sources, (act, weight, bias, out, mods), scratch = refs[:count], refs[count:count + 5], refs[count + 5:]
    peers = Peers()
    peers.barrier()
    tiles, stages, scratch = Stream(*scratch[:TWO]), Stream(*scratch[TWO:ZS]), scratch[ZS:]

    def tile(i):
        product = dot_cols(act[...], tiles.ready(i))
        stages.store(i, (product + bias[:, tile_at(i)]).astype(BF16), mods.at[:, tile_at(i)])

    fill = Filler([Job(TILES, tile, lambda i: tiles.load(i, weight.at[tile_at(i)]))], TWO)
    fill.prime()
    own = len(AllGather.scratch)
    rs = ReduceScatter(peers, sources, pieces, split, scratch[own:])
    rs.run(fill)
    fill.finish()
    AllGather(peers, rs.part.at[peers.z, peers.y, peers.x], out, split, scratch[:own]).run()
    rs.drain()
    stages.drain()


def reduce_all(sources, pieces, act, weight, bias):
    split = Split(*EMBED_SPLIT)
    return pl.pallas_call(
        functools.partial(reduce_kernel, pieces, split, len(sources)),
        out_shape=[jax.ShapeDtypeStruct((ZS, TWO, TWO, TWO, split.rows, WIDTH), F32), jax.ShapeDtypeStruct((ROWS, MOD), BF16)],
        in_specs=[ANY] * len(sources) + [IN_VMEM, ANY, IN_VMEM], out_specs=[ANY, ANY],
        scratch_shapes=[*Stream.scratch(BF16, TILE, WIDTH), *Stream.scratch(BF16, ROWS, TILE), *AllGather.scratch, *ReduceScatter.scratch(split)],
        compiler_params=comm_params(TWO), name="reduce_embed",
    )(*sources, act, weight, bias)


def unpack_kernel(pieces, total, *refs):
    *outs, buf, load_sem, store_sem = refs
    order = [(zp, core) for zp in range(ZS) for core in range(TWO)]
    for at in order:
        local(total.at[at[0], :, :, at[1]], buf.at[at], load_sem.at[at])
    for at in order:
        wait_for(buf.at[at], load_sem.at[at])
        zp, core = at
        for dst, start, n, row in pieces[core]:
            local(buf.at[zp, core, :, :, pl.ds(row, n)], outs[dst].at[zp, :, :, pl.ds(start, n)], store_sem.at[at])
    for at in order:
        wait_for(buf.at[at], store_sem.at[at])


def unpack(total, sources, pieces):
    return pl.pallas_call(
        functools.partial(unpack_kernel, pieces),
        out_shape=[jax.ShapeDtypeStruct(s.shape, s.dtype) for s in sources],
        in_specs=[ANY], out_specs=[ANY] * len(sources),
        scratch_shapes=[pltpu.VMEM((ZS, TWO, TWO, TWO, *total.shape[ZS:]), F32), DMA((ZS, TWO)), DMA((ZS, TWO))],
        compiler_params=pltpu.CompilerParams(vmem_limit_bytes=VMEM_LIMIT), name="unpack",
    )(total)


def compact_kernel(blocks, out):
    for k in range(ZS):
        out[k * SHARE:(k + 1) * SHARE] = blocks[k, :SHARE]


def compact(blocks):
    return pl.pallas_call(
        compact_kernel,
        grid=(DEVICES // ZS,),
        out_shape=jax.ShapeDtypeStruct((MOD, WIDTH), BF16),
        in_specs=[pl.BlockSpec((ZS, PADDED, WIDTH), lambda i: (i, 0, 0))],
        out_specs=pl.BlockSpec((ZS * SHARE, WIDTH), lambda i: (i, 0)),
        compiler_params=pltpu.CompilerParams(vmem_limit_bytes=VMEM_LIMIT), name="compact",
    )(blocks)


def sinusoid(values, freq_width):
    half_width = freq_width // 2
    freq_table = jnp.exp(-math.log(MAX_PERIOD) * jnp.arange(half_width, dtype=F32) / half_width)
    angles = (TIME_SCALE * values)[:, None] * freq_table[None, :]
    return jnp.concatenate([jnp.cos(angles), jnp.sin(angles)], axis=1).astype(BF16)


def silu_grad(values):
    sigmoid_v = jax.nn.sigmoid(values)
    return sigmoid_v * (1.0 + values * (1.0 - sigmoid_v))


def mlp_forward(inputs_bf, params):
    hidden = jnp.dot(inputs_bf, params[0], preferred_element_type=F32) + params[1].astype(F32)
    act_bf = jax.nn.silu(hidden).astype(BF16)
    output = jnp.dot(act_bf, params[2], preferred_element_type=F32) + params[3].astype(F32)
    return output, hidden, act_bf


def by_chip(grad):
    return grad.reshape(ZS, TWO, TWO, grad.shape[0] // CHIPS, WIDTH)


WGRAD_PIECES = (((0, 0, 184, 0),), ((0, 176, 184, 0),))
EMBED_PIECES = (
    ((0, 0, 16, 0), (1, 0, 16, 16), (2, 0, 128, 32), (6, 0, 8, 160), (3, 0, 24, 168)),
    ((3, 24, 48, 0), (4, 0, 72, 48), (5, 0, 72, 120)),
)


def solution(mesh):
    row_split = P(AXIS)
    row_matrix = P(AXIS, None)
    col_matrix = P(None, AXIS)
    embed_specs = (P(None, None), P(None), P(None, None), P(None)) * 3
    in_specs = (row_split, row_split, row_matrix) + embed_specs + (col_matrix, row_split, row_matrix)
    out_specs = (row_matrix, col_matrix, row_split) + embed_specs

    def local_step(timesteps, guidance, pooled, time_w1, time_b1, time_w2, time_b2, guide_w1, guide_b1, guide_w2, guide_b2, text_w1, text_b1, text_w2, text_b2, w_mod, b_mod, d_mods):
        me = lax.axis_index(AXIS)
        freq_width = time_w1.shape[0]
        inputs_list = [sinusoid(timesteps, freq_width), sinusoid(guidance, freq_width), pooled]
        params_list = [(time_w1, time_b1, time_w2, time_b2), (guide_w1, guide_b1, guide_w2, guide_b2), (text_w1, text_b1, text_w2, text_b2)]
        saved = [mlp_forward(u, params) for u, params in zip(inputs_list, params_list)]
        cond_vec = saved[0][0] + saved[1][0] + saved[2][0]
        cond_silu = jax.nn.silu(cond_vec).astype(BF16)

        extra = jnp.pad(b_mod[None, :], ((0, PADDED - SHARE - 1), (0, WIDTH - SHARE)))
        gathered, part_wgrad = gather_blocks(jnp.concatenate([w_mod.T, extra], axis=0), d_mods, cond_silu)
        gathered = gathered.reshape(DEVICES, PADDED, WIDTH)
        full_wt = compact(gathered)
        full_b = gathered[:, SHARE, :SHARE].reshape(1, MOD).astype(F32)
        hidden, acts = [record[1] for record in saved], [record[2] for record in saved]
        second = [params[TWO] for params in params_list]
        wgrad, sums, *grads = scatter_sum(by_chip(part_wgrad), d_mods, full_wt, cond_vec, hidden, second, inputs_list, acts, WGRAD_PIECES)
        grad_wmod = lax.dynamic_slice(wgrad, (4 * lax.rem(me, TWO), 0), (SHARE, WIDTH)).T
        bgrad_rows, count = MOD // WIDTH, len(hidden)
        part_bgrad = jnp.sum(d_mods, axis=0, dtype=F32).reshape(bgrad_rows, WIDTH)
        vectors = jnp.concatenate([sums[:ZS], part_bgrad], axis=0)
        vectors = jnp.pad(vectors, ((0, 128 - vectors.shape[0]), (0, 0)))
        sources = [by_chip(g) for g in (*grads, vectors)]
        total, modulation = reduce_all(sources, EMBED_PIECES, cond_silu, full_wt, full_b)
        *full, sums = [g.reshape(-1, WIDTH) for g in unpack(total, sources, EMBED_PIECES)]
        grad_bmod = lax.dynamic_slice(sums[ZS:ZS + bgrad_rows].reshape(MOD), (SHARE * me,), (SHARE,))
        embed_grads = [g for i in range(count) for g in (full[i], sums[i], full[i + count], sums[count])]
        return (modulation, grad_wmod, grad_bmod, *embed_grads)

    return jax.shard_map(local_step, mesh=mesh, in_specs=in_specs, out_specs=out_specs, check_vma=False)
```

```python
import functools
import math
import jax
import jax.numpy as jnp
from jax import lax
from jax.experimental import pallas as pl
from jax.experimental.pallas import tpu as pltpu
from jax.sharding import PartitionSpec as P

AXIS = "fsdp"
MESH = pl.DeviceIdType.MESH
MAX_PERIOD = 10000.0
TIME_SCALE = 1000.0
CONTRACT_ROWS = (((0,), (0,)), ((), ()))
CONTRACT_COLS = (((1,), (1,)), ((), ()))
F32, BF16 = jnp.float32, jnp.bfloat16
VMEM_LIMIT = 62 << 20
TWO, ZS, CHIPS, DEVICES = 2, 4, 16, 32
ROWS, WIDTH, MOD, SHARE, PADDED = 512, 1152, 5760, 180, 184
TILE, TILES = 384, 15
Z_ORDER = (3, 0, 2, 1)
ANY = pl.BlockSpec(memory_space=pl.ANY)
IN_VMEM = pl.BlockSpec(memory_space=pltpu.VMEM)
DMA = pltpu.SemaphoreType.DMA
WMOD_SPLIT = (80, 64, 16, 24)
WGRAD_SPLIT = (72, 72, 24, 16)
EMBED_SPLIT = (80, 72, 24, 16)


class Peers:
    def __init__(self):
        me = lax.axis_index(AXIS)
        bits = []
        for _ in range(3):
            bits.append(lax.rem(me, TWO))
            me = lax.div(me, TWO)
        self.c, self.x, self.y = bits
        self.oc, self.ox, self.oy = (1 - bit for bit in bits)
        self.z = me
        self.core = self.device(me, self.y, self.x, self.oc)
        self.xn = self.device(me, self.y, self.ox, self.c)
        self.yn = self.device(me, self.oy, self.x, self.c)

    def device(self, z, y, x, c):
        return (((z * TWO + y) * TWO + x) * TWO + c,)

    def column(self, zp):
        return self.device(zp, self.y, self.x, self.c)

    def elsewhere(self, fn):
        for zp in range(ZS):
            pl.when(self.z != zp)(functools.partial(fn, zp))

    def barrier(self):
        sem = pltpu.get_barrier_semaphore()

        def greet(peer):
            pl.semaphore_signal(sem, device_id=peer, device_id_type=MESH)

        for peer in (self.core, self.xn, self.yn):
            greet(peer)
        self.elsewhere(lambda zp: greet(self.column(zp)))
        pl.semaphore_wait(sem, 6)


def remote(src, dst, sems, peer):
    pltpu.make_async_remote_copy(src_ref=src, dst_ref=dst, send_sem=sems[0], recv_sem=sems[1], device_id=peer, device_id_type=MESH).start()


def local(src, dst, sem):
    pltpu.make_async_copy(src, dst, sem).start()


def wait_for(ref, sem):
    pltpu.make_async_copy(ref, ref, sem).wait()


def add_rows(dst, src):
    if len(dst.shape) > TWO:
        for i in range(dst.shape[0]):
            add_rows(dst.at[i], src.at[i])
        return
    rows = dst.shape[0]
    step = 24 if rows % 24 == 0 else 8

    def body(i, carry):
        at = pl.ds(pl.multiple_of(i * step, 8), step)
        dst[at, :] = dst[at, :] + src[at, :]
        return carry

    lax.fori_loop(0, rows // step, body, 0)


class Sems:
    def __init__(self, refs, *index):
        self.send, self.recv, self.index = *refs, index

    def __getitem__(self, k):
        return self.send.at[(*self.index, k)], self.recv.at[(*self.index, k)]

    def under(self, k):
        return Sems((self.send, self.recv), *self.index, k)

    @staticmethod
    def scratch(*shape):
        return [DMA(shape), DMA(shape)]


class Split:
    def __init__(self, *n):
        starts = [sum(n[:i]) for i in range(ZS)]
        ranges = [pl.ds(start, size) for start, size in zip(starts, n)]
        self.n, self.colours = (n[:TWO], n[TWO:]), (ranges[:TWO], ranges[TWO:])
        self.a, self.b = sum(self.n[0]), sum(self.n[1])
        self.rows = self.a + self.b
        self.all_a, self.all_b = pl.ds(0, self.a), pl.ds(self.a, self.b)
        size = -(-self.a // DEVICES) * 8
        self.chunks = [pl.ds(at, min(size, self.a - at)) for at in range(0, self.a, size)]


class PlaneReduce:
    @staticmethod
    def shapes(sizes):
        one, two = sizes
        return [(TWO, one), (TWO, two), (one,), (two,)]

    def __init__(self, p, plane, colours, boxes, sems):
        one, two = colours
        x1, y1, y2, x2 = boxes
        self.sems = sems
        self.moves = (
            (plane.at[:, p.ox, one], x1, p.xn), (plane.at[p.oy, :, two], y1, p.yn),
            (plane.at[p.oy, p.x, one], y2, p.yn), (plane.at[p.y, p.ox, two], x2, p.xn),
        )
        mine = plane.at[p.y, p.x]
        self.first = ((x1.at[p.oy], x1.at[p.y]), (y1.at[p.ox], y1.at[p.x]))
        self.mine = (mine.at[one], mine.at[two])

    def send(self, k):
        src, dst, peer = self.moves[k]
        remote(src, dst, self.sems[k], peer)

    def got(self, k):
        wait_for(self.moves[k][1], self.sems[k][1])

    def start(self):
        for k in range(TWO):
            self.send(k)

    def middle(self):
        for k in range(TWO):
            self.got(k)
            add_rows(self.moves[k + TWO][0], self.first[k][0])
            self.send(k + TWO)
        for k in range(TWO):
            add_rows(self.mine[k], self.first[k][1])

    def end(self):
        for k in range(TWO):
            self.got(k + TWO)
            add_rows(self.mine[k], self.moves[k + TWO][1])

    def drain(self):
        for k, move in enumerate(self.moves):
            wait_for(move[1], self.sems[k][0])


class ReduceScatter:
    @staticmethod
    def scratch(s):
        whole = [(n, TWO, TWO, s.rows) for n in (ZS, TWO)]
        planes = [(ZS,) + shape for shape in PlaneReduce.shapes(s.n[0])] + PlaneReduce.shapes(s.n[1])
        shapes = whole + planes + [(TWO, ZS, s.a), (ZS, TWO, TWO, s.b)]
        buffers = [pltpu.VMEM(shape + (WIDTH,), F32) for shape in shapes]
        return buffers + [DMA((ZS,))] + Sems.scratch(ZS) + Sems.scratch(ZS, ZS) + Sems.scratch(TWO, ZS, len(s.chunks)) + Sems.scratch(ZS) + Sems.scratch(ZS)

    def __init__(self, p, sources, pieces, s, scratch):
        self.p, self.sources, self.pieces, self.s = p, sources, pieces, s
        scratch = list(scratch)
        take = lambda n: [scratch.pop(0) for _ in range(n)]
        self.part, self.own = take(TWO)
        boxes, slab_boxes = take(ZS), take(ZS)
        self.line, self.slabs, self.lsem = take(3)
        self.csems, plane_sems, self.zsems, self.bsems, slab_sems = (Sems(take(TWO)) for _ in range(5))
        self.planes = [PlaneReduce(p, self.part.at[zp], s.colours[0], [box.at[zp] for box in boxes], plane_sems.under(zp)) for zp in range(ZS)]
        self.slab = PlaneReduce(p, self.part.at[p.z], s.colours[1], slab_boxes, slab_sems)

    def partner(self, zp):
        def send(core):
            for src, start, n, at in self.pieces[1 - core]:
                remote(self.sources[src].at[zp, :, :, pl.ds(start, n)], self.part.at[zp, :, :, pl.ds(at, n)], self.csems[zp], self.p.core)

        self.by_core(send)

    def load(self, zp):
        slot = Z_ORDER.index(zp) % TWO

        def start(core):
            for src, at_src, n, at in self.pieces[core]:
                local(self.sources[src].at[zp, :, :, pl.ds(at_src, n)], self.own.at[slot, :, :, pl.ds(at, n)], self.lsem.at[zp])

        self.by_core(start)

    def by_core(self, fn):
        for core in range(TWO):
            pl.when(self.p.c == core)(functools.partial(fn, core))

    def both_cores(self, zp):
        own = self.own.at[Z_ORDER.index(zp) % TWO]
        wait_for(own, self.lsem.at[zp])
        wait_for(self.part.at[zp], self.csems[zp][1])
        add_rows(self.part.at[zp], own)

    def slab_out(self, zp):
        p = self.p

        @pl.when(p.z != zp)
        def _():
            sems = self.bsems[zp][0], self.bsems[p.z][1]
            remote(self.part.at[zp, :, :, self.s.all_b], self.slabs.at[p.z], sems, p.column(zp))

    def slab_sum(self, zp):
        wait_for(self.slabs.at[zp], self.bsems[zp][1])
        add_rows(self.part.at[self.p.z, :, :, self.s.all_b], self.slabs.at[zp])

    def line_in(self, way, zp, k, part):
        box = self.line.at[way, zp, part]
        wait_for(box, self.zsems.under(way).under(zp)[k][1])
        add_rows(self.part.at[zp, self.p.y, self.p.x, part], box)

    def hop(self, zp, distance):
        p = self.p

        def go(way, step):
            for k, part in enumerate(self.s.chunks):
                if distance:
                    self.line_in(way, zp, k, part)
                remote(self.part.at[zp, p.y, p.x, part], self.line.at[way, zp, part], self.zsems.under(way).under(zp)[k], p.column(p.z + step))

        last = ZS - 1
        for way, (step, at, todo) in enumerate(((1, distance, distance < zp), (-1, last - distance, last - distance > zp))):
            if todo:
                pl.when(p.z == at)(functools.partial(go, way, step))

    def final(self, zp):
        @pl.when(self.p.z == zp)
        def _():
            for k, part in enumerate(self.s.chunks):
                for way, end in enumerate((0, ZS - 1)):
                    if zp != end:
                        self.line_in(way, zp, k, part)

    def drain(self):
        p = self.p
        self.slab.drain()
        p.elsewhere(lambda zp: wait_for(self.slabs.at[zp], self.bsems[zp][0]))

        def sent(way, zp):
            for k, part in enumerate(self.s.chunks):
                wait_for(self.line.at[way, zp, part], self.zsems.under(way).under(zp)[k][0])

        for zp in range(ZS):
            wait_for(self.part.at[zp], self.csems[zp][0])
            self.planes[zp].drain()
            for way, cond in enumerate((p.z < zp, p.z > zp)):
                pl.when(cond)(functools.partial(sent, way, zp))

    def run(self, fill=lambda: None):
        one, two, three, four = Z_ORDER
        planes = self.planes
        for zp in Z_ORDER:
            self.partner(zp)
        self.load(one)
        self.load(two)
        fill()
        for zp, later in zip(Z_ORDER, (three, four, None, None)):
            self.both_cores(zp)
            if later is None:
                self.slab_out(zp)
            else:
                self.load(later)
                planes[zp].start()
                self.slab_out(zp)
            fill()
        planes[one].middle()
        planes[three].start()
        fill()
        planes[one].end()
        self.hop(one, 0)
        fill()
        planes[two].middle()
        planes[four].start()
        fill()
        planes[two].end()
        self.hop(two, 0)
        self.hop(one, 1)
        fill()
        planes[three].middle()
        fill()
        planes[three].end()
        self.hop(three, 0)
        self.hop(two, 1)
        self.hop(one, TWO)
        fill()
        self.p.elsewhere(self.slab_sum)
        self.slab.start()
        fill()
        planes[four].middle()
        self.slab.middle()
        fill()
        planes[four].end()
        self.hop(four, 0)
        self.hop(three, 1)
        self.hop(two, TWO)
        self.hop(four, 1)
        self.slab.end()
        fill()
        for zp in Z_ORDER:
            self.final(zp)


class PlaneGather:
    def __init__(self, p, plane, colours, sems):
        one, two = colours
        mine, ynb, xnb, far = (plane.at[y, x, p.c] for y, x in ((p.y, p.x), (p.oy, p.x), (p.y, p.ox), (p.oy, p.ox)))
        self.mine, self.blocks, self.sems = mine, (ynb, xnb, far), sems
        self.moves = ((mine, one, p.yn), (mine, two, p.xn), (mine, two, p.yn), (mine, one, p.xn), (ynb, one, p.xn), (xnb, two, p.yn))

    def send(self, k, src=None):
        block, at, peer = self.moves[k]
        remote((block if src is None else src).at[at], block.at[at], self.sems[k], peer)

    def got(self, k, side=1):
        block, at, peer = self.moves[k]
        wait_for(block.at[at], self.sems[k][side])

    def start(self, src):
        for k in range(ZS):
            self.send(k, src)

    def relay(self):
        for k in range(TWO):
            self.got(k)
            self.send(k + ZS)

    def rest(self, forward=None):
        waits = ((TWO,), (3,), (ZS, 5))
        for ks, block in zip(waits, self.blocks):
            for k in ks:
                self.got(k)
            if forward is not None:
                forward(block)

    def drain(self):
        for k in range(len(self.moves)):
            self.got(k, 0)


class AllGather:
    scratch = [*Sems.scratch(TWO, ZS), *Sems.scratch(ZS, 6), *Sems.scratch(ZS), *Sems.scratch(ZS), *Sems.scratch(6), DMA]

    def __init__(self, p, own, out, s, scratch):
        self.p, self.own, self.out, self.s = p, own, out, s
        *pairs, self.lsem = scratch
        self.zsems, self.plane_sems, self.csems, self.bsems, slab_sems = (Sems(pair) for pair in zip(pairs[::TWO], pairs[1::TWO]))
        self.slab = PlaneGather(p, out.at[p.z], s.colours[1], slab_sems)

    def plane(self, zp):
        return PlaneGather(self.p, self.out.at[zp], self.s.colours[0], self.plane_sems.under(zp))

    def band(self, zp):
        return self.out.at[zp, :, :, self.p.c, self.s.all_b]

    def forward(self, zp, src, dst):
        remote(src, dst, self.csems[zp], self.p.core)

    def spread(self, zp, src):
        plane, a = self.plane(zp), self.s.all_a
        plane.start(src)
        self.forward(zp, src.at[a], plane.mine.at[a])

    def send_z(self, way, zp, src):
        p = self.p
        step, end = ((1, ZS - 1), (-1, 0))[way]

        @pl.when(p.z != end)
        def _():
            remote(src, self.plane(zp).mine.at[self.s.all_a], self.zsems.under(way)[zp], p.column(p.z + step))

    def arrive(self, way, zp):
        mine = self.plane(zp).mine
        part = mine.at[self.s.all_a]
        wait_for(part, self.zsems.under(way)[zp][1])
        self.send_z(way, zp, part)
        self.spread(zp, mine)

    def relay(self, way, zp):
        self.plane(zp).relay()

    def finish(self, way, zp):
        def forward(block):
            part = block.at[self.s.all_a]
            self.forward(zp, part, part)

        self.plane(zp).rest(forward)

    def at_distance(self, d, *fns):
        z = self.p.z
        for fn in fns:
            if d:
                pl.when(z >= d)(functools.partial(fn, 0, z - d))
                pl.when(z + d < ZS)(functools.partial(fn, 1, z + d))
            else:
                fn(0, z)

    def band_out(self):
        p, band = self.p, self.band(self.p.z)
        self.forward(p.z, band, band)
        p.elsewhere(lambda zp: remote(band, band, (self.bsems[zp][0], self.bsems[p.z][1]), p.column(zp)))

    def band_in(self, zp):
        band = self.band(zp)
        wait_for(band, self.bsems[zp][1])
        self.forward(zp, band, band)

    def run(self, fill=lambda: None):
        p = self.p
        local(self.own, self.slab.mine, self.lsem)
        self.slab.start(self.own)
        for way in range(TWO):
            self.send_z(way, p.z, self.own.at[self.s.all_a])
        self.spread(p.z, self.own)
        fill()
        self.slab.relay()
        wait_for(self.own, self.lsem)
        near, mid, far = range(1, ZS)
        self.at_distance(0, self.relay)
        fill()
        self.at_distance(near, self.arrive)
        fill()
        self.at_distance(mid, self.arrive)
        self.slab.rest()
        self.band_out()
        self.at_distance(0, self.finish)
        fill()
        self.at_distance(near, self.relay)
        fill()
        self.at_distance(far, self.arrive)
        fill()
        self.at_distance(near, self.finish)
        fill()
        self.at_distance(mid, self.relay)
        fill()
        self.at_distance(mid, self.finish)
        fill()
        self.at_distance(far, self.relay)
        fill()
        p.elsewhere(self.band_in)
        fill()
        self.at_distance(far, self.finish)
        self.slab.drain()
        p.elsewhere(lambda zp: wait_for(self.band(zp), self.bsems[zp][0]))
        part = self.slab.mine.at[self.s.all_a]

        def sent(way, zp):
            wait_for(part, self.zsems.under(way)[zp][0])

        for zp in range(ZS):
            for sem in self.csems[zp]:
                wait_for(self.out.at[zp, :, :, p.c], sem)
            self.plane(zp).drain()
            for way, cond in enumerate(((p.z < ZS - 1) & (p.z >= zp), (p.z > 0) & (p.z <= zp))):
                pl.when(cond)(functools.partial(sent, way, zp))


class Job:
    def __init__(self, count, body, load=None, close=None):
        self.count, self.body, self.load, self.close = count, body, load, close


class Filler:
    def __init__(self, jobs, share):
        self.jobs, self.share, self.job, self.at = jobs, share, 0, 0

    def prime(self):
        self.jobs[0].load(0)

    def part(self, stop):
        job, last = self.jobs[self.job], self.jobs[self.job].count - 1
        after = next((j.load for j in self.jobs[self.job + 1:] if j.load), None)

        def next_job():
            if job.close:
                job.close()
            if after:
                after(0)

        def tile(i, carry):
            if job.load:
                @pl.when(i < last)
                def _():
                    job.load(i + 1)

                if not job.close:
                    pl.when(i == last)(next_job)
            job.body(i)
            if job.close:
                pl.when(i == last)(next_job)
            return carry

        lax.fori_loop(self.at, stop, tile, 0)

    def __call__(self):
        left = self.share
        while left and self.job < len(self.jobs):
            count = self.jobs[self.job].count
            stop = min(self.at + left, count)
            self.part(stop)
            left -= stop - self.at
            self.at = stop
            if stop == count:
                self.job, self.at = self.job + 1, 0

    def finish(self):
        while self.job < len(self.jobs):
            self()


class Stream:
    def __init__(self, buf, sems, base=0):
        self.buf, self.sems, self.base = buf, sems, base

    def slot(self, i):
        return lax.rem(i + self.base, TWO)

    def load(self, i, src):
        slot = self.slot(i)
        local(src, self.buf.at[slot], self.sems.at[slot])

    def ready(self, i):
        slot = self.slot(i)
        wait_for(self.buf.at[slot], self.sems.at[slot])
        return self.buf[slot]

    def free(self, i):
        pl.when(i + self.base >= TWO)(lambda: wait_for(self.buf.at[self.slot(i)], self.sems.at[self.slot(i)]))

    def store(self, i, value, dst):
        slot = self.slot(i)
        self.free(i)
        self.buf[slot] = value
        local(self.buf.at[slot], dst, self.sems.at[slot])

    def drain(self):
        for slot in range(TWO):
            wait_for(self.buf.at[slot], self.sems.at[slot])

    def trim(self, *at):
        return Stream(self.buf.at[(slice(None), *at)], self.sems)

    def after(self, count):
        return Stream(self.buf, self.sems, self.base + count)

    @staticmethod
    def scratch(dtype, *shape):
        return [pltpu.VMEM((TWO, *shape), dtype), DMA((TWO,))]


def tile_at(i, width=TILE, start=0):
    return pl.ds(pl.multiple_of(start + i * width, 16 if width % 128 else 128), width)


def dot_rows(left, right):
    return lax.dot_general(left, right, CONTRACT_ROWS, preferred_element_type=F32)


def dot_cols(left, right):
    return lax.dot_general(left, right, CONTRACT_COLS, preferred_element_type=F32)


def comm_params(ident):
    return pltpu.CompilerParams(collective_id=ident, has_side_effects=True, vmem_limit_bytes=VMEM_LIMIT)


def gather_kernel(split, mlps, own, d_mods, biases, *refs):
    refs = list(refs)
    take = lambda n: [refs.pop(0) for _ in range(n)]
    sources = [d_mods, *take(3 * mlps)]
    out, wgrad, bgrad = take(3)
    results, hidden = take(mlps + TWO), take(mlps)
    mods, *weights = take(len(sources))
    kept = take(len(results))
    cvec, act, *acts = kept
    load_sem, keep_sem = take(TWO)
    inputs, first, second = weights[:mlps], weights[mlps:TWO * mlps], weights[TWO * mlps:]
    tiles, stages = Stream(*take(TWO)), Stream(*take(TWO))
    pairs = list(zip(sources, [mods, *weights]))
    for n, (src, dst) in enumerate(pairs[1:] + pairs[:1]):
        local(src, dst, load_sem.at[n])
    peers = Peers()
    peers.barrier()

    def ready(i, buf, n):
        pl.when(i == 0)(lambda: wait_for(buf, load_sem.at[n]))

    jobs = []
    per = WIDTH // TILE
    for k in range(mlps):
        def hide(i, k=k, stage=stages.after(k * per)):
            ready(i, inputs[k], k)
            ready(i, first[k], k + mlps)
            value = jnp.dot(inputs[k][...], first[k][:, tile_at(i)], preferred_element_type=F32) + biases[k:k + 1, tile_at(i)]
            stage.store(i, value, hidden[k].at[:, tile_at(i)])
            acts[k][:, tile_at(i)] = jax.nn.silu(value).astype(BF16)

        jobs.append(Job(per, hide))
    for k in range(mlps):
        def embed(i, k=k):
            ready(i, second[k], k + TWO * mlps)
            value = jnp.dot(acts[k][...], second[k][:, tile_at(i)], preferred_element_type=F32) + biases[k + mlps:k + mlps + 1, tile_at(i)]
            cvec[:, tile_at(i)] = cvec[:, tile_at(i)] + value if k else value

        jobs.append(Job(per, embed))

    def activate(i):
        at = tile_at(i, ROWS // ZS)
        act[at, :] = jax.nn.silu(cvec[at, :]).astype(BF16)

    def keep():
        for n, (src, dst) in enumerate(zip(kept, results)):
            local(src, dst, keep_sem.at[n])

    def tile(i):
        ready(i, mods, len(weights))
        left = mods[:, tile_at(i)]
        bgrad[:, tile_at(i)] = jnp.sum(left.astype(F32), axis=0, keepdims=True)
        tiles.store(i, dot_rows(left, act[...]), wgrad.at[tile_at(i)])

    fill = Filler(jobs + [Job(ZS, activate, close=keep), Job(TILES, tile)], 3)
    AllGather(peers, own, out, split, refs).run(fill)
    fill.finish()
    tiles.drain()
    stages.drain()
    for n, buf in enumerate(kept):
        wait_for(buf, keep_sem.at[n])


def gather_blocks(block, d_mods, biases, inputs, first, second):
    split, mlps = Split(*WMOD_SPLIT), len(inputs)
    sources = [*inputs, *first, *second]
    wide = (ROWS, WIDTH)
    kept = [(wide, F32)] + [(wide, BF16)] * (mlps + 1)
    shapes = [(MOD, WIDTH), (1, MOD)]
    return pl.pallas_call(
        functools.partial(gather_kernel, split, mlps),
        out_shape=[jax.ShapeDtypeStruct((ZS, TWO, TWO, TWO, split.rows, WIDTH), block.dtype)]
        + [jax.ShapeDtypeStruct(shape, F32) for shape in shapes] + [jax.ShapeDtypeStruct(*k) for k in kept] + [jax.ShapeDtypeStruct(wide, F32)] * mlps,
        in_specs=[ANY, ANY, IN_VMEM] + [ANY] * len(sources), out_specs=[ANY, ANY, IN_VMEM] + [ANY] * (len(kept) + mlps),
        scratch_shapes=[
            *(pltpu.VMEM(a.shape, BF16) for a in (d_mods, *sources)), *(pltpu.VMEM(*k) for k in kept), DMA((len(sources) + 1,)), DMA((len(kept),)),
            *Stream.scratch(F32, TILE, WIDTH), *Stream.scratch(F32, ROWS, TILE), *AllGather.scratch,
        ],
        compiler_params=comm_params(0), name="gather_wmod",
    )(block, d_mods, biases, *sources)


def scatter_kernel(pieces, split, mlps, *refs):
    refs = list(refs)
    take = lambda n: [refs.pop(0) for _ in range(n)]
    source, d_mods, blocks, cond = take(ZS)
    hidden, second, inputs, acts = (take(mlps) for _ in range(ZS))
    out, sums, weight = take(3)
    grads1, grads2 = take(mlps), take(mlps)
    mods, dcond, sem, mods_sem = take(ZS)
    wtiles, htiles, ltiles, stiles, padded, packed = (Stream(*take(TWO)) for _ in range(6))
    small = inputs[0].shape[1]
    lsmall, ssmall = ltiles.trim(slice(None), pl.ds(0, small)), stiles.trim(pl.ds(0, small))
    local(d_mods, mods, mods_sem)
    peers = Peers()
    peers.barrier()
    rs = ReduceScatter(peers, [source], pieces, split, refs)

    def vector(k):
        return mods.at[:, pl.ds(k * WIDTH, WIDTH)]

    def d_cond(i):
        @pl.when(i == 0)
        def _():
            wait_for(mods, mods_sem)

        product = jnp.dot(mods[:, tile_at(i)], wtiles.ready(i), preferred_element_type=F32)
        dcond[...] = jnp.where(i == 0, 0.0, dcond[...]) + product

    def d_vec(i):
        @pl.when(i == 0)
        def _():
            sums[...] = jnp.zeros_like(sums)

        at = tile_at(i)
        value = dcond[:, at] * silu_grad(htiles.ready(i))
        mods[:, at] = value.astype(BF16)
        sums[mlps:mlps + 1, at] = jnp.sum(value, axis=0, keepdims=True)

    def pack(i):
        slot = packed.slot(i)
        padded.ready(i)
        packed.free(i)
        for k in range(ZS):
            packed.buf[slot, k * SHARE:(k + 1) * SHARE] = padded.buf[slot, k, :SHARE]
        local(packed.buf.at[slot], weight.at[tile_at(i, ZS * SHARE)], packed.sems.at[slot])

    per = WIDTH // TILE
    jobs = [Job(DEVICES // ZS, pack, lambda i: padded.load(i, blocks.at[pl.ds(i * ZS, ZS)]), packed.drain)]
    jobs += [Job(TILES, d_cond, lambda i: wtiles.load(i, weight.at[tile_at(i)])), Job(per, d_vec, lambda i: htiles.load(i, cond.at[:, tile_at(i)]))]
    for k in range(mlps):
        w, h = wtiles.after(TILES + k * per), htiles.after((k + 1) * per)

        def load(i, k=k, w=w, h=h):
            w.load(i, second[k].at[tile_at(i)])
            h.load(i, hidden[k].at[:, tile_at(i)])

        def d_hidden(i, k=k, w=w, h=h):
            value = dot_cols(vector(0)[...], w.ready(i)) * silu_grad(h.ready(i))
            mods[:, tile_at(i, start=(k + 1) * WIDTH)] = value.astype(BF16)
            sums[k:k + 1, tile_at(i)] = jnp.sum(value, axis=0, keepdims=True)

        jobs.append(Job(per, d_hidden, load))

    def outer(count, left, right, dst, lefts, stages, width, close=None):
        def load(i):
            lefts.load(i, left.at[:, tile_at(i, width)])

        def body(i):
            stages.store(i, dot_rows(lefts.ready(i), right[...]), dst.at[tile_at(i, width)])

        jobs.append(Job(count, body, load, close))

    done = 0
    for k in range(mlps):
        outer(per, acts[k], vector(0), grads2[k], ltiles.after(k * per), stiles.after(k * per), TILE, stiles.drain if k == mlps - 1 else None)
    for k in range(mlps):
        count = inputs[k].shape[1] // small
        outer(count, inputs[k], vector(k + 1), grads1[k], lsmall.after(done), ssmall.after(done), small)
        done += count
    fill = Filler(jobs, ZS)
    fill.prime()
    rs.run(fill)
    local(rs.part.at[peers.z, peers.y, peers.x], out, sem)
    fill.finish()
    ssmall.drain()
    rs.drain()
    wait_for(out, sem)


def scatter_sum(partial, d_mods, blocks, cond, hidden, second, inputs, acts, pieces):
    split = Split(*WGRAD_SPLIT)
    args = [partial, d_mods, blocks, cond, *hidden, *second, *inputs, *acts]
    grads = [jax.ShapeDtypeStruct((a.shape[1], WIDTH), F32) for a in (*inputs, *acts)]
    return pl.pallas_call(
        functools.partial(scatter_kernel, pieces, split, len(hidden)),
        out_shape=[jax.ShapeDtypeStruct((split.rows, WIDTH), F32), jax.ShapeDtypeStruct((8, WIDTH), F32), jax.ShapeDtypeStruct((MOD, WIDTH), BF16), *grads],
        in_specs=[ANY] * len(args), out_specs=[ANY, IN_VMEM] + [ANY] * (len(grads) + 1),
        scratch_shapes=[
            pltpu.VMEM(d_mods.shape, BF16), pltpu.VMEM(cond.shape, F32), DMA, DMA,
            *Stream.scratch(BF16, TILE, WIDTH), *Stream.scratch(F32, ROWS, TILE), *Stream.scratch(BF16, ROWS, TILE), *Stream.scratch(F32, TILE, WIDTH),
            *Stream.scratch(BF16, ZS, PADDED, WIDTH), *Stream.scratch(BF16, ZS * SHARE, WIDTH), *ReduceScatter.scratch(split),
        ],
        compiler_params=comm_params(1), name="scatter_wgrad",
    )(*args)


def reduce_kernel(pieces, split, count, *refs):
    sources, out, scratch = refs[:count], refs[count], refs[count + 1:]
    peers = Peers()
    peers.barrier()
    own = len(AllGather.scratch)
    rs = ReduceScatter(peers, sources, pieces, split, scratch[own:])
    rs.run()
    AllGather(peers, rs.part.at[peers.z, peers.y, peers.x], out, split, scratch[:own]).run()
    rs.drain()


def reduce_all(sources, pieces):
    split = Split(*EMBED_SPLIT)
    return pl.pallas_call(
        functools.partial(reduce_kernel, pieces, split, len(sources)),
        out_shape=jax.ShapeDtypeStruct((ZS, TWO, TWO, TWO, split.rows, WIDTH), F32),
        in_specs=[ANY] * len(sources), out_specs=ANY, scratch_shapes=[*AllGather.scratch, *ReduceScatter.scratch(split)],
        compiler_params=comm_params(TWO), name="reduce_embed",
    )(*sources)


def unpack_kernel(pieces, total, act, weight, bias, *refs):
    mods, *outs, buf, load_sem, store_sem = refs[:-ZS]
    tiles, stages = Stream(*refs[-ZS:-TWO]), Stream(*refs[-TWO:])

    def tile(i):
        product = dot_cols(act[...], tiles.ready(i))
        stages.store(i, (product + bias[:, tile_at(i)]).astype(BF16), mods.at[:, tile_at(i)])

    fill = Filler([Job(TILES, tile, lambda i: tiles.load(i, weight.at[tile_at(i)]))], TWO)
    fill.prime()
    order = [(zp, core) for zp in range(ZS) for core in range(TWO)]
    for at in order:
        local(total.at[at[0], :, :, at[1]], buf.at[at], load_sem.at[at])
    for at in order:
        wait_for(buf.at[at], load_sem.at[at])
        zp, core = at
        for dst, start, n, row in pieces[core]:
            local(buf.at[zp, core, :, :, pl.ds(row, n)], outs[dst].at[zp, :, :, pl.ds(start, n)], store_sem.at[at])
        fill()
    fill.finish()
    stages.drain()
    for at in order:
        wait_for(buf.at[at], store_sem.at[at])


def unpack(total, sources, pieces, act, weight, bias):
    return pl.pallas_call(
        functools.partial(unpack_kernel, pieces),
        out_shape=[jax.ShapeDtypeStruct((ROWS, MOD), BF16)] + [jax.ShapeDtypeStruct(s.shape, s.dtype) for s in sources],
        in_specs=[ANY, IN_VMEM, ANY, IN_VMEM], out_specs=[ANY] * (len(sources) + 1),
        scratch_shapes=[
            pltpu.VMEM((ZS, TWO, TWO, TWO, *total.shape[ZS:]), F32), DMA((ZS, TWO)), DMA((ZS, TWO)),
            *Stream.scratch(BF16, TILE, WIDTH), *Stream.scratch(BF16, ROWS, TILE),
        ],
        compiler_params=pltpu.CompilerParams(vmem_limit_bytes=VMEM_LIMIT), name="unpack",
    )(total, act, weight, bias)


def sinusoid(values, freq_width):
    half_width = freq_width // 2
    freq_table = jnp.exp(-math.log(MAX_PERIOD) * jnp.arange(half_width, dtype=F32) / half_width)
    angles = (TIME_SCALE * values)[:, None] * freq_table[None, :]
    return jnp.concatenate([jnp.cos(angles), jnp.sin(angles)], axis=1).astype(BF16)


def silu_grad(values):
    sigmoid_v = jax.nn.sigmoid(values)
    return sigmoid_v * (1.0 + values * (1.0 - sigmoid_v))


def by_chip(grad):
    return grad.reshape(ZS, TWO, TWO, grad.shape[0] // CHIPS, WIDTH)


WGRAD_PIECES = (((0, 0, 184, 0),), ((0, 176, 184, 0),))
EMBED_PIECES = (
    ((0, 0, 16, 0), (1, 0, 16, 16), (2, 0, 128, 32), (6, 0, 8, 160), (3, 0, 24, 168)),
    ((3, 24, 48, 0), (4, 0, 72, 48), (5, 0, 72, 120)),
)


def solution(mesh):
    row_split = P(AXIS)
    row_matrix = P(AXIS, None)
    col_matrix = P(None, AXIS)
    embed_specs = (P(None, None), P(None), P(None, None), P(None)) * 3
    in_specs = (row_split, row_split, row_matrix) + embed_specs + (col_matrix, row_split, row_matrix)
    out_specs = (row_matrix, col_matrix, row_split) + embed_specs

    def local_step(timesteps, guidance, pooled, time_w1, time_b1, time_w2, time_b2, guide_w1, guide_b1, guide_w2, guide_b2, text_w1, text_b1, text_w2, text_b2, w_mod, b_mod, d_mods):
        me = lax.axis_index(AXIS)
        freq_width = time_w1.shape[0]
        inputs_list = [sinusoid(timesteps, freq_width), sinusoid(guidance, freq_width), pooled]
        first, second = [time_w1, guide_w1, text_w1], [time_w2, guide_w2, text_w2]
        count = len(first)
        biases = jnp.stack([time_b1, guide_b1, text_b1, time_b2, guide_b2, text_b2]).astype(F32)
        extra = jnp.pad(b_mod[None, :], ((0, PADDED - SHARE - 1), (0, WIDTH - SHARE)))
        block = jnp.concatenate([w_mod.T, extra], axis=0)
        gathered, part_wgrad, part_bgrad, cond_vec, cond_silu, *rest = gather_blocks(block, d_mods, biases, inputs_list, first, second)
        acts, hidden = rest[:count], rest[count:]
        gathered = gathered.reshape(DEVICES, PADDED, WIDTH)
        full_b = gathered[:, SHARE, :SHARE].reshape(1, MOD).astype(F32)
        wgrad, sums, full_wt, *grads = scatter_sum(by_chip(part_wgrad), d_mods, gathered, cond_vec, hidden, second, inputs_list, acts, WGRAD_PIECES)
        grad_wmod = lax.dynamic_slice(wgrad, (4 * lax.rem(me, TWO), 0), (SHARE, WIDTH)).T
        bgrad_rows = MOD // WIDTH
        part_bgrad = part_bgrad.reshape(bgrad_rows, WIDTH)
        vectors = jnp.concatenate([sums[:ZS], part_bgrad], axis=0)
        vectors = jnp.pad(vectors, ((0, 128 - vectors.shape[0]), (0, 0)))
        sources = [by_chip(g) for g in (*grads, vectors)]
        total = reduce_all(sources, EMBED_PIECES)
        modulation, *full = unpack(total, sources, EMBED_PIECES, cond_silu, full_wt, full_b)
        *full, sums = [g.reshape(-1, WIDTH) for g in full]
        grad_bmod = lax.dynamic_slice(sums[ZS:ZS + bgrad_rows].reshape(MOD), (SHARE * me,), (SHARE,))
        embed_grads = [g for i in range(count) for g in (full[i], sums[i], full[i + count], sums[count])]
        return (modulation, grad_wmod, grad_bmod, *embed_grads)

    return jax.shard_map(local_step, mesh=mesh, in_specs=in_specs, out_specs=out_specs, check_vma=False)
```

```python
import functools
import math
import jax
import jax.numpy as jnp
from jax import lax
from jax.experimental import pallas as pl
from jax.experimental.pallas import tpu as pltpu
from jax.sharding import PartitionSpec as P

AXIS = "fsdp"
MESH = pl.DeviceIdType.MESH
MAX_PERIOD = 10000.0
TIME_SCALE = 1000.0
CONTRACT_ROWS = (((0,), (0,)), ((), ()))
CONTRACT_COLS = (((1,), (1,)), ((), ()))
F32, BF16 = jnp.float32, jnp.bfloat16
VMEM_LIMIT = 62 << 20
TWO, ZS, CHIPS, DEVICES = 2, 4, 16, 32
ROWS, WIDTH, MOD, SHARE, PADDED = 512, 1152, 5760, 180, 184
TILE, TILES = 384, 15
Z_ORDER = (3, 0, 2, 1)
ANY = pl.BlockSpec(memory_space=pl.ANY)
IN_VMEM = pl.BlockSpec(memory_space=pltpu.VMEM)
DMA = pltpu.SemaphoreType.DMA
WMOD_SPLIT = (80, 64, 16, 24)
WGRAD_SPLIT = (72, 72, 24, 16)
EMBED_SPLIT = (80, 72, 24, 16)


class Peers:
    def __init__(self):
        me = lax.axis_index(AXIS)
        bits = []
        for _ in range(3):
            bits.append(lax.rem(me, TWO))
            me = lax.div(me, TWO)
        self.c, self.x, self.y = bits
        self.oc, self.ox, self.oy = (1 - bit for bit in bits)
        self.z = me
        self.core = self.device(me, self.y, self.x, self.oc)
        self.xn = self.device(me, self.y, self.ox, self.c)
        self.yn = self.device(me, self.oy, self.x, self.c)

    def device(self, z, y, x, c):
        return (((z * TWO + y) * TWO + x) * TWO + c,)

    def column(self, zp):
        return self.device(zp, self.y, self.x, self.c)

    def elsewhere(self, fn):
        for zp in range(ZS):
            pl.when(self.z != zp)(functools.partial(fn, zp))

    def barrier(self):
        sem = pltpu.get_barrier_semaphore()

        def greet(peer):
            pl.semaphore_signal(sem, device_id=peer, device_id_type=MESH)

        for peer in (self.core, self.xn, self.yn):
            greet(peer)
        self.elsewhere(lambda zp: greet(self.column(zp)))
        pl.semaphore_wait(sem, 6)


def remote(src, dst, sems, peer):
    pltpu.make_async_remote_copy(src_ref=src, dst_ref=dst, send_sem=sems[0], recv_sem=sems[1], device_id=peer, device_id_type=MESH).start()


def local(src, dst, sem):
    pltpu.make_async_copy(src, dst, sem).start()


def wait_for(ref, sem):
    pltpu.make_async_copy(ref, ref, sem).wait()


def add_rows(dst, src):
    if len(dst.shape) > TWO:
        for i in range(dst.shape[0]):
            add_rows(dst.at[i], src.at[i])
        return
    rows = dst.shape[0]
    step = 24 if rows % 24 == 0 else 8

    def body(i, carry):
        at = pl.ds(pl.multiple_of(i * step, 8), step)
        dst[at, :] = dst[at, :] + src[at, :]
        return carry

    lax.fori_loop(0, rows // step, body, 0)


class Sems:
    def __init__(self, refs, *index):
        self.send, self.recv, self.index = *refs, index

    def __getitem__(self, k):
        return self.send.at[(*self.index, k)], self.recv.at[(*self.index, k)]

    def under(self, k):
        return Sems((self.send, self.recv), *self.index, k)

    @staticmethod
    def scratch(*shape):
        return [DMA(shape), DMA(shape)]


def halves(start, size):
    one = -(-size // CHIPS) * 8
    return pl.ds(start, one), pl.ds(start + one, size - one)


class Split:
    def __init__(self, *n):
        starts = [sum(n[:i]) for i in range(ZS)]
        ranges = [pl.ds(start, size) for start, size in zip(starts, n)]
        self.n, self.colours = (n[:TWO], n[TWO:]), (ranges[:TWO], ranges[TWO:])
        self.a, self.b = sum(self.n[0]), sum(self.n[1])
        self.rows = self.a + self.b
        self.all_a, self.all_b = pl.ds(0, self.a), pl.ds(self.a, self.b)
        self.units = [halves(start, size) for start, size in zip(starts, self.n[0])]


class PlaneReduce:
    @staticmethod
    def shapes(sizes):
        one, two = sizes
        return [(TWO, one), (TWO, two), (one,), (two,)]

    def __init__(self, p, plane, colours, boxes, sems):
        one, two = colours
        x1, y1, y2, x2 = boxes
        self.sems = sems
        self.moves = (
            (plane.at[:, p.ox, one], x1, p.xn), (plane.at[p.oy, :, two], y1, p.yn),
            (plane.at[p.oy, p.x, one], y2, p.yn), (plane.at[p.y, p.ox, two], x2, p.xn),
        )
        mine = plane.at[p.y, p.x]
        self.first = ((x1.at[p.oy], x1.at[p.y]), (y1.at[p.ox], y1.at[p.x]))
        self.mine = (mine.at[one], mine.at[two])

    def send(self, k):
        src, dst, peer = self.moves[k]
        remote(src, dst, self.sems[k], peer)

    def got(self, k):
        wait_for(self.moves[k][1], self.sems[k][1])

    def start(self):
        for k in range(TWO):
            self.send(k)

    def middle(self):
        for k in range(TWO):
            self.got(k)
            add_rows(self.moves[k + TWO][0], self.first[k][0])
            self.send(k + TWO)
        for k in range(TWO):
            add_rows(self.mine[k], self.first[k][1])

    def end(self):
        for k in range(TWO):
            self.got(k + TWO)
            add_rows(self.mine[k], self.moves[k + TWO][1])

    def drain(self):
        for k, move in enumerate(self.moves):
            wait_for(move[1], self.sems[k][0])


class ReduceScatter:
    @staticmethod
    def scratch(s):
        whole = [(n, TWO, TWO, s.rows) for n in (ZS, TWO)]
        planes = [(ZS,) + shape for unit in s.units for shape in PlaneReduce.shapes([at.size for at in unit])] + PlaneReduce.shapes(s.n[1])
        shapes = whole + planes + [(TWO, ZS, s.a), (ZS, TWO, TWO, s.b)]
        buffers = [pltpu.VMEM(shape + (WIDTH,), F32) for shape in shapes]
        return buffers + [DMA((ZS,))] + Sems.scratch(ZS) + Sems.scratch(ZS, TWO, ZS) + Sems.scratch(TWO, ZS, TWO, TWO) + Sems.scratch(ZS) + Sems.scratch(ZS)

    def __init__(self, p, sources, pieces, s, scratch):
        self.p, self.sources, self.pieces, self.s = p, sources, pieces, s
        scratch = list(scratch)
        take = lambda n: [scratch.pop(0) for _ in range(n)]
        self.part, self.own = take(TWO)
        boxes, slab_boxes = [take(ZS) for _ in s.units], take(ZS)
        self.line, self.slabs, self.lsem = take(3)
        self.csems, plane_sems, self.zsems, self.bsems, slab_sems = (Sems(take(TWO)) for _ in range(5))
        self.planes = {
            (zp, n): PlaneReduce(p, self.part.at[zp], unit, [box.at[zp] for box in boxes[n]], plane_sems.under(zp).under(n))
            for zp in range(ZS) for n, unit in enumerate(s.units)
        }
        self.slab = PlaneReduce(p, self.part.at[p.z], s.colours[1], slab_boxes, slab_sems)

    def partner(self, zp):
        def send(core):
            for src, start, n, at in self.pieces[1 - core]:
                remote(self.sources[src].at[zp, :, :, pl.ds(start, n)], self.part.at[zp, :, :, pl.ds(at, n)], self.csems[zp], self.p.core)

        self.by_core(send)

    def load(self, zp):
        slot = Z_ORDER.index(zp) % TWO

        def start(core):
            for src, at_src, n, at in self.pieces[core]:
                local(self.sources[src].at[zp, :, :, pl.ds(at_src, n)], self.own.at[slot, :, :, pl.ds(at, n)], self.lsem.at[zp])

        self.by_core(start)

    def by_core(self, fn):
        for core in range(TWO):
            pl.when(self.p.c == core)(functools.partial(fn, core))

    def both_cores(self, zp):
        own = self.own.at[Z_ORDER.index(zp) % TWO]
        wait_for(own, self.lsem.at[zp])
        wait_for(self.part.at[zp], self.csems[zp][1])
        add_rows(self.part.at[zp], own)

    def slab_out(self, zp):
        p = self.p

        @pl.when(p.z != zp)
        def _():
            sems = self.bsems[zp][0], self.bsems[p.z][1]
            remote(self.part.at[zp, :, :, self.s.all_b], self.slabs.at[p.z], sems, p.column(zp))

    def slab_sum(self, zp):
        wait_for(self.slabs.at[zp], self.bsems[zp][1])
        add_rows(self.part.at[self.p.z, :, :, self.s.all_b], self.slabs.at[zp])

    def line_in(self, way, zp, n, k, part):
        box = self.line.at[way, zp, part]
        wait_for(box, self.zsems.under(way).under(zp).under(n)[k][1])
        add_rows(self.part.at[zp, self.p.y, self.p.x, part], box)

    def hop(self, unit, distance):
        p, (zp, n) = self.p, unit

        def go(way, step):
            for k, part in enumerate(self.s.units[n]):
                if distance:
                    self.line_in(way, zp, n, k, part)
                remote(self.part.at[zp, p.y, p.x, part], self.line.at[way, zp, part], self.zsems.under(way).under(zp).under(n)[k], p.column(p.z + step))

        last = ZS - 1
        for way, (step, at, todo) in enumerate(((1, distance, distance < zp), (-1, last - distance, last - distance > zp))):
            if todo:
                pl.when(p.z == at)(functools.partial(go, way, step))

    def final(self, zp, n):
        @pl.when(self.p.z == zp)
        def _():
            for k, part in enumerate(self.s.units[n]):
                for way, end in enumerate((0, ZS - 1)):
                    if zp != end:
                        self.line_in(way, zp, n, k, part)

    def drain(self):
        p = self.p
        self.slab.drain()
        p.elsewhere(lambda zp: wait_for(self.slabs.at[zp], self.bsems[zp][0]))

        def sent(way, zp):
            for n, unit in enumerate(self.s.units):
                for k, part in enumerate(unit):
                    wait_for(self.line.at[way, zp, part], self.zsems.under(way).under(zp).under(n)[k][0])

        for zp in range(ZS):
            wait_for(self.part.at[zp], self.csems[zp][0])
            for n in range(TWO):
                self.planes[zp, n].drain()
            for way, cond in enumerate((p.z < zp, p.z > zp)):
                pl.when(cond)(functools.partial(sent, way, zp))

    def run(self, fill, lag):
        units = [(zp, n) for zp in Z_ORDER for n in range(TWO)]
        planes = [self.planes[unit] for unit in units]
        for zp in Z_ORDER:
            self.partner(zp)
        for zp in Z_ORDER[:TWO]:
            self.load(zp)
        fill()
        ahead = 3
        for n, zp in enumerate(Z_ORDER):
            self.both_cores(zp)
            for plane in planes[n * TWO:min(n * TWO + TWO, ahead)]:
                plane.start()
            self.slab_out(zp)
            for later in Z_ORDER[TWO:][n:n + 1]:
                self.load(later)
            fill()
        last = len(units) - 1
        for u, plane in enumerate(planes):
            plane.middle()
            for later in planes[u + ahead:u + ahead + 1]:
                later.start()
            if u == last:
                self.slab.middle()
            fill()
            plane.end()
            for distance, unit in enumerate(units[u::-lag][:3]):
                self.hop(unit, distance)
            if u == last - 1:
                self.p.elsewhere(self.slab_sum)
                self.slab.start()
            fill()
        for unit in units[-lag:]:
            self.hop(unit, 1)
        self.slab.end()
        fill()
        for unit in units:
            self.final(*unit)


class PlaneGather:
    def __init__(self, p, plane, colours, sems):
        one, two = colours
        mine, ynb, xnb, far = (plane.at[y, x, p.c] for y, x in ((p.y, p.x), (p.oy, p.x), (p.y, p.ox), (p.oy, p.ox)))
        self.mine, self.blocks, self.sems = mine, (ynb, xnb, far), sems
        self.moves = ((mine, one, p.yn), (mine, two, p.xn), (mine, two, p.yn), (mine, one, p.xn), (ynb, one, p.xn), (xnb, two, p.yn))

    def send(self, k, src=None):
        block, at, peer = self.moves[k]
        remote((block if src is None else src).at[at], block.at[at], self.sems[k], peer)

    def got(self, k, side=1):
        block, at, peer = self.moves[k]
        wait_for(block.at[at], self.sems[k][side])

    def start(self, src):
        for k in range(ZS):
            self.send(k, src)

    def relay(self):
        for k in range(TWO):
            self.got(k)
            self.send(k + ZS)

    def rest(self, forward=None):
        waits = ((TWO,), (3,), (ZS, 5))
        for ks, block in zip(waits, self.blocks):
            for k in ks:
                self.got(k)
            if forward is not None:
                forward(block)

    def drain(self):
        for k in range(len(self.moves)):
            self.got(k, 0)


class AllGather:
    scratch = [*Sems.scratch(TWO, ZS), *Sems.scratch(ZS, 6), *Sems.scratch(ZS), *Sems.scratch(ZS), *Sems.scratch(6), DMA]

    def __init__(self, p, own, out, s, scratch):
        self.p, self.own, self.out, self.s = p, own, out, s
        *pairs, self.lsem = scratch
        self.zsems, self.plane_sems, self.csems, self.bsems, slab_sems = (Sems(pair) for pair in zip(pairs[::TWO], pairs[1::TWO]))
        self.slab = PlaneGather(p, out.at[p.z], s.colours[1], slab_sems)

    def plane(self, zp):
        return PlaneGather(self.p, self.out.at[zp], self.s.colours[0], self.plane_sems.under(zp))

    def band(self, zp):
        return self.out.at[zp, :, :, self.p.c, self.s.all_b]

    def forward(self, zp, src, dst):
        remote(src, dst, self.csems[zp], self.p.core)

    def spread(self, zp, src):
        plane, a = self.plane(zp), self.s.all_a
        plane.start(src)
        self.forward(zp, src.at[a], plane.mine.at[a])

    def send_z(self, way, zp, src):
        p = self.p
        step, end = ((1, ZS - 1), (-1, 0))[way]

        @pl.when(p.z != end)
        def _():
            remote(src, self.plane(zp).mine.at[self.s.all_a], self.zsems.under(way)[zp], p.column(p.z + step))

    def arrive(self, way, zp):
        mine = self.plane(zp).mine
        part = mine.at[self.s.all_a]
        wait_for(part, self.zsems.under(way)[zp][1])
        self.send_z(way, zp, part)
        self.spread(zp, mine)

    def relay(self, way, zp):
        self.plane(zp).relay()

    def finish(self, way, zp):
        def forward(block):
            part = block.at[self.s.all_a]
            self.forward(zp, part, part)

        self.plane(zp).rest(forward)

    def at_distance(self, d, *fns):
        z = self.p.z
        for fn in fns:
            if d:
                pl.when(z >= d)(functools.partial(fn, 0, z - d))
                pl.when(z + d < ZS)(functools.partial(fn, 1, z + d))
            else:
                fn(0, z)

    def band_out(self):
        p, band = self.p, self.band(self.p.z)
        self.forward(p.z, band, band)
        p.elsewhere(lambda zp: remote(band, band, (self.bsems[zp][0], self.bsems[p.z][1]), p.column(zp)))

    def band_in(self, zp):
        band = self.band(zp)
        wait_for(band, self.bsems[zp][1])
        self.forward(zp, band, band)

    def run(self, fill=lambda: None):
        p = self.p
        local(self.own, self.slab.mine, self.lsem)
        self.slab.start(self.own)
        for way in range(TWO):
            self.send_z(way, p.z, self.own.at[self.s.all_a])
        self.spread(p.z, self.own)
        fill()
        self.slab.relay()
        wait_for(self.own, self.lsem)
        near, mid, far = range(1, ZS)
        self.at_distance(0, self.relay)
        fill()
        self.at_distance(near, self.arrive)
        fill()
        self.at_distance(mid, self.arrive)
        self.slab.rest()
        self.band_out()
        self.at_distance(0, self.finish)
        fill()
        self.at_distance(near, self.relay)
        fill()
        self.at_distance(far, self.arrive)
        fill()
        self.at_distance(near, self.finish)
        fill()
        self.at_distance(mid, self.relay)
        fill()
        self.at_distance(mid, self.finish)
        fill()
        self.at_distance(far, self.relay)
        fill()
        p.elsewhere(self.band_in)
        fill()
        self.at_distance(far, self.finish)
        self.slab.drain()
        p.elsewhere(lambda zp: wait_for(self.band(zp), self.bsems[zp][0]))
        part = self.slab.mine.at[self.s.all_a]

        def sent(way, zp):
            wait_for(part, self.zsems.under(way)[zp][0])

        for zp in range(ZS):
            for sem in self.csems[zp]:
                wait_for(self.out.at[zp, :, :, p.c], sem)
            self.plane(zp).drain()
            for way, cond in enumerate(((p.z < ZS - 1) & (p.z >= zp), (p.z > 0) & (p.z <= zp))):
                pl.when(cond)(functools.partial(sent, way, zp))


class Job:
    def __init__(self, count, body, load=None, close=None):
        self.count, self.body, self.load, self.close = count, body, load, close


class Filler:
    def __init__(self, jobs, share):
        self.jobs, self.share, self.job, self.at = jobs, share, 0, 0

    def prime(self):
        self.jobs[0].load(0)

    def part(self, stop):
        job, last = self.jobs[self.job], self.jobs[self.job].count - 1
        after = next((j.load for j in self.jobs[self.job + 1:] if j.load), None)

        def next_job():
            if job.close:
                job.close()
            if after:
                after(0)

        def tile(i, carry):
            if job.load:
                @pl.when(i < last)
                def _():
                    job.load(i + 1)

                if not job.close:
                    pl.when(i == last)(next_job)
            job.body(i)
            if job.close:
                pl.when(i == last)(next_job)
            return carry

        lax.fori_loop(self.at, stop, tile, 0)

    def __call__(self):
        left = self.share
        while left and self.job < len(self.jobs):
            count = self.jobs[self.job].count
            stop = min(self.at + left, count)
            self.part(stop)
            left -= stop - self.at
            self.at = stop
            if stop == count:
                self.job, self.at = self.job + 1, 0

    def finish(self):
        while self.job < len(self.jobs):
            self()


class Stream:
    def __init__(self, buf, sems, base=0):
        self.buf, self.sems, self.base = buf, sems, base

    def slot(self, i):
        return lax.rem(i + self.base, TWO)

    def load(self, i, src):
        slot = self.slot(i)
        local(src, self.buf.at[slot], self.sems.at[slot])

    def ready(self, i):
        slot = self.slot(i)
        wait_for(self.buf.at[slot], self.sems.at[slot])
        return self.buf[slot]

    def free(self, i):
        pl.when(i + self.base >= TWO)(lambda: wait_for(self.buf.at[self.slot(i)], self.sems.at[self.slot(i)]))

    def store(self, i, value, dst):
        slot = self.slot(i)
        self.free(i)
        self.buf[slot] = value
        local(self.buf.at[slot], dst, self.sems.at[slot])

    def drain(self):
        for slot in range(TWO):
            wait_for(self.buf.at[slot], self.sems.at[slot])

    def trim(self, *at):
        return Stream(self.buf.at[(slice(None), *at)], self.sems)

    def after(self, count):
        return Stream(self.buf, self.sems, self.base + count)

    @staticmethod
    def scratch(dtype, *shape):
        return [pltpu.VMEM((TWO, *shape), dtype), DMA((TWO,))]


def tile_at(i, width=TILE, start=0):
    return pl.ds(pl.multiple_of(start + i * width, 16 if width % 128 else 128), width)


def dot_rows(left, right):
    return lax.dot_general(left, right, CONTRACT_ROWS, preferred_element_type=F32)


def dot_cols(left, right):
    return lax.dot_general(left, right, CONTRACT_COLS, preferred_element_type=F32)


def comm_params(ident):
    return pltpu.CompilerParams(collective_id=ident, has_side_effects=True, vmem_limit_bytes=VMEM_LIMIT)


def gather_kernel(split, mlps, own, d_mods, biases, *refs):
    refs = list(refs)
    take = lambda n: [refs.pop(0) for _ in range(n)]
    sources = [d_mods, *take(3 * mlps)]
    out, wgrad, bgrad = take(3)
    results, hidden = take(mlps + TWO), take(mlps)
    mods, *weights = take(len(sources))
    kept = take(len(results))
    cvec, act, *acts = kept
    load_sem, keep_sem = take(TWO)
    inputs, first, second = weights[:mlps], weights[mlps:TWO * mlps], weights[TWO * mlps:]
    tiles, stages = Stream(*take(TWO)), Stream(*take(TWO))
    pairs = list(zip(sources, [mods, *weights]))
    for n, (src, dst) in enumerate(pairs[1:] + pairs[:1]):
        local(src, dst, load_sem.at[n])
    peers = Peers()
    peers.barrier()

    def ready(i, buf, n):
        pl.when(i == 0)(lambda: wait_for(buf, load_sem.at[n]))

    jobs = []
    per = WIDTH // TILE
    for k in range(mlps):
        def hide(i, k=k, stage=stages.after(k * per)):
            ready(i, inputs[k], k)
            ready(i, first[k], k + mlps)
            value = jnp.dot(inputs[k][...], first[k][:, tile_at(i)], preferred_element_type=F32) + biases[k:k + 1, tile_at(i)]
            stage.store(i, value, hidden[k].at[:, tile_at(i)])
            acts[k][:, tile_at(i)] = jax.nn.silu(value).astype(BF16)

        jobs.append(Job(per, hide))
    for k in range(mlps):
        def embed(i, k=k):
            ready(i, second[k], k + TWO * mlps)
            value = jnp.dot(acts[k][...], second[k][:, tile_at(i)], preferred_element_type=F32) + biases[k + mlps:k + mlps + 1, tile_at(i)]
            cvec[:, tile_at(i)] = cvec[:, tile_at(i)] + value if k else value

        jobs.append(Job(per, embed))

    def activate(i):
        at = tile_at(i, ROWS // ZS)
        act[at, :] = jax.nn.silu(cvec[at, :]).astype(BF16)

    def keep():
        for n, (src, dst) in enumerate(zip(kept, results)):
            local(src, dst, keep_sem.at[n])

    def tile(i):
        ready(i, mods, len(weights))
        left = mods[:, tile_at(i)]
        bgrad[:, tile_at(i)] = jnp.sum(left.astype(F32), axis=0, keepdims=True)
        tiles.store(i, dot_rows(left, act[...]), wgrad.at[tile_at(i)])

    fill = Filler(jobs + [Job(ZS, activate, close=keep), Job(TILES, tile)], 3)
    AllGather(peers, own, out, split, refs).run(fill)
    fill.finish()
    tiles.drain()
    stages.drain()
    for n, buf in enumerate(kept):
        wait_for(buf, keep_sem.at[n])


def gather_blocks(block, d_mods, biases, inputs, first, second):
    split, mlps = Split(*WMOD_SPLIT), len(inputs)
    sources = [*inputs, *first, *second]
    wide = (ROWS, WIDTH)
    kept = [(wide, F32)] + [(wide, BF16)] * (mlps + 1)
    shapes = [(MOD, WIDTH), (1, MOD)]
    return pl.pallas_call(
        functools.partial(gather_kernel, split, mlps),
        out_shape=[jax.ShapeDtypeStruct((ZS, TWO, TWO, TWO, split.rows, WIDTH), block.dtype)]
        + [jax.ShapeDtypeStruct(shape, F32) for shape in shapes] + [jax.ShapeDtypeStruct(*k) for k in kept] + [jax.ShapeDtypeStruct(wide, F32)] * mlps,
        in_specs=[ANY, ANY, IN_VMEM] + [ANY] * len(sources), out_specs=[ANY, ANY, IN_VMEM] + [ANY] * (len(kept) + mlps),
        scratch_shapes=[
            *(pltpu.VMEM(a.shape, BF16) for a in (d_mods, *sources)), *(pltpu.VMEM(*k) for k in kept), DMA((len(sources) + 1,)), DMA((len(kept),)),
            *Stream.scratch(F32, TILE, WIDTH), *Stream.scratch(F32, ROWS, TILE), *AllGather.scratch,
        ],
        compiler_params=comm_params(0), name="gather_wmod",
    )(block, d_mods, biases, *sources)


def scatter_kernel(pieces, split, mlps, *refs):
    refs = list(refs)
    take = lambda n: [refs.pop(0) for _ in range(n)]
    source, d_mods, blocks, cond = take(ZS)
    hidden, second, inputs, acts = (take(mlps) for _ in range(ZS))
    out, sums, weight = take(3)
    grads1, grads2 = take(mlps), take(mlps)
    mods, dcond, sem, mods_sem = take(ZS)
    wtiles, htiles, ltiles, stiles, padded, packed = (Stream(*take(TWO)) for _ in range(6))
    small = inputs[0].shape[1]
    lsmall, ssmall = ltiles.trim(slice(None), pl.ds(0, small)), stiles.trim(pl.ds(0, small))
    local(d_mods, mods, mods_sem)
    peers = Peers()
    peers.barrier()
    rs = ReduceScatter(peers, [source], pieces, split, refs)

    def vector(k):
        return mods.at[:, pl.ds(k * WIDTH, WIDTH)]

    def d_cond(i):
        @pl.when(i == 0)
        def _():
            wait_for(mods, mods_sem)

        product = jnp.dot(mods[:, tile_at(i)], wtiles.ready(i), preferred_element_type=F32)
        dcond[...] = jnp.where(i == 0, 0.0, dcond[...]) + product

    def d_vec(i):
        @pl.when(i == 0)
        def _():
            sums[...] = jnp.zeros_like(sums)

        at = tile_at(i)
        value = dcond[:, at] * silu_grad(htiles.ready(i))
        mods[:, at] = value.astype(BF16)
        sums[mlps:mlps + 1, at] = jnp.sum(value, axis=0, keepdims=True)

    def pack(i):
        slot = packed.slot(i)
        padded.ready(i)
        packed.free(i)
        for k in range(ZS):
            packed.buf[slot, k * SHARE:(k + 1) * SHARE] = padded.buf[slot, k, :SHARE]
        local(packed.buf.at[slot], weight.at[tile_at(i, ZS * SHARE)], packed.sems.at[slot])

    per = WIDTH // TILE
    jobs = [Job(DEVICES // ZS, pack, lambda i: padded.load(i, blocks.at[pl.ds(i * ZS, ZS)]), packed.drain)]
    jobs += [Job(TILES, d_cond, lambda i: wtiles.load(i, weight.at[tile_at(i)])), Job(per, d_vec, lambda i: htiles.load(i, cond.at[:, tile_at(i)]))]
    for k in range(mlps):
        w, h = wtiles.after(TILES + k * per), htiles.after((k + 1) * per)

        def load(i, k=k, w=w, h=h):
            w.load(i, second[k].at[tile_at(i)])
            h.load(i, hidden[k].at[:, tile_at(i)])

        def d_hidden(i, k=k, w=w, h=h):
            value = dot_cols(vector(0)[...], w.ready(i)) * silu_grad(h.ready(i))
            mods[:, tile_at(i, start=(k + 1) * WIDTH)] = value.astype(BF16)
            sums[k:k + 1, tile_at(i)] = jnp.sum(value, axis=0, keepdims=True)

        jobs.append(Job(per, d_hidden, load))

    def outer(count, left, right, dst, lefts, stages, width, close=None):
        def load(i):
            lefts.load(i, left.at[:, tile_at(i, width)])

        def body(i):
            stages.store(i, dot_rows(lefts.ready(i), right[...]), dst.at[tile_at(i, width)])

        jobs.append(Job(count, body, load, close))

    done = 0
    for k in range(mlps):
        outer(per, acts[k], vector(0), grads2[k], ltiles.after(k * per), stiles.after(k * per), TILE, stiles.drain if k == mlps - 1 else None)
    for k in range(mlps):
        count = inputs[k].shape[1] // small
        outer(count, inputs[k], vector(k + 1), grads1[k], lsmall.after(done), ssmall.after(done), small)
        done += count
    fill = Filler(jobs, ZS)
    fill.prime()
    rs.run(fill, TWO)
    local(rs.part.at[peers.z, peers.y, peers.x], out, sem)
    fill.finish()
    ssmall.drain()
    rs.drain()
    wait_for(out, sem)


def scatter_sum(partial, d_mods, blocks, cond, hidden, second, inputs, acts, pieces):
    split = Split(*WGRAD_SPLIT)
    args = [partial, d_mods, blocks, cond, *hidden, *second, *inputs, *acts]
    grads = [jax.ShapeDtypeStruct((a.shape[1], WIDTH), F32) for a in (*inputs, *acts)]
    return pl.pallas_call(
        functools.partial(scatter_kernel, pieces, split, len(hidden)),
        out_shape=[jax.ShapeDtypeStruct((split.rows, WIDTH), F32), jax.ShapeDtypeStruct((8, WIDTH), F32), jax.ShapeDtypeStruct((MOD, WIDTH), BF16), *grads],
        in_specs=[ANY] * len(args), out_specs=[ANY, IN_VMEM] + [ANY] * (len(grads) + 1),
        scratch_shapes=[
            pltpu.VMEM(d_mods.shape, BF16), pltpu.VMEM(cond.shape, F32), DMA, DMA,
            *Stream.scratch(BF16, TILE, WIDTH), *Stream.scratch(F32, ROWS, TILE), *Stream.scratch(BF16, ROWS, TILE), *Stream.scratch(F32, TILE, WIDTH),
            *Stream.scratch(BF16, ZS, PADDED, WIDTH), *Stream.scratch(BF16, ZS * SHARE, WIDTH), *ReduceScatter.scratch(split),
        ],
        compiler_params=comm_params(1), name="scatter_wgrad",
    )(*args)


def reduce_kernel(pieces, split, count, *refs):
    sources, (act, weight, bias, out, mods), scratch = refs[:count], refs[count:count + 5], refs[count + 5:]
    peers = Peers()
    peers.barrier()
    tiles, stages, scratch = Stream(*scratch[:TWO]), Stream(*scratch[TWO:ZS]), scratch[ZS:]

    def tile(i):
        product = dot_cols(act[...], tiles.ready(i))
        stages.store(i, (product + bias[:, tile_at(i)]).astype(BF16), mods.at[:, tile_at(i)])

    fill = Filler([Job(TILES, tile, lambda i: tiles.load(i, weight.at[tile_at(i)]))], 1)
    fill.prime()
    own = len(AllGather.scratch)
    rs = ReduceScatter(peers, sources, pieces, split, scratch[own:])
    rs.run(fill, TWO)
    fill.finish()
    AllGather(peers, rs.part.at[peers.z, peers.y, peers.x], out, split, scratch[:own]).run()
    rs.drain()
    stages.drain()


def reduce_all(sources, pieces, act, weight, bias):
    split = Split(*EMBED_SPLIT)
    return pl.pallas_call(
        functools.partial(reduce_kernel, pieces, split, len(sources)),
        out_shape=[jax.ShapeDtypeStruct((ZS, TWO, TWO, TWO, split.rows, WIDTH), F32), jax.ShapeDtypeStruct((ROWS, MOD), BF16)],
        in_specs=[ANY] * len(sources) + [IN_VMEM, ANY, IN_VMEM], out_specs=[ANY, ANY],
        scratch_shapes=[*Stream.scratch(BF16, TILE, WIDTH), *Stream.scratch(BF16, ROWS, TILE), *AllGather.scratch, *ReduceScatter.scratch(split)],
        compiler_params=comm_params(TWO), name="reduce_embed",
    )(*sources, act, weight, bias)


def unpack_kernel(pieces, total, mods, *refs):
    final_mods, *outs, buf, mods_buf, load_sem, store_sem, mods_sem = refs
    order = [(zp, core) for zp in range(ZS) for core in range(TWO)]
    local(mods, mods_buf, mods_sem.at[0])
    for at in order:
        local(total.at[at[0], :, :, at[1]], buf.at[at], load_sem.at[at])
    wait_for(mods_buf, mods_sem.at[0])
    local(mods_buf, final_mods, mods_sem.at[1])
    for at in order:
        wait_for(buf.at[at], load_sem.at[at])
        zp, core = at
        for dst, start, n, row in pieces[core]:
            local(buf.at[zp, core, :, :, pl.ds(row, n)], outs[dst].at[zp, :, :, pl.ds(start, n)], store_sem.at[at])
    for at in order:
        wait_for(buf.at[at], store_sem.at[at])
    wait_for(mods_buf, mods_sem.at[1])


def unpack(total, mods, sources, pieces):
    return pl.pallas_call(
        functools.partial(unpack_kernel, pieces),
        out_shape=[jax.ShapeDtypeStruct(s.shape, s.dtype) for s in (mods, *sources)],
        in_specs=[ANY, ANY], out_specs=[ANY] * (len(sources) + 1),
        scratch_shapes=[
            pltpu.VMEM((ZS, TWO, TWO, TWO, *total.shape[ZS:]), F32), pltpu.VMEM(mods.shape, BF16), DMA((ZS, TWO)), DMA((ZS, TWO)), DMA((TWO,)),
        ],
        compiler_params=pltpu.CompilerParams(vmem_limit_bytes=VMEM_LIMIT), name="unpack",
    )(total, mods)


def sinusoid(values, freq_width):
    half_width = freq_width // 2
    freq_table = jnp.exp(-math.log(MAX_PERIOD) * jnp.arange(half_width, dtype=F32) / half_width)
    angles = (TIME_SCALE * values)[:, None] * freq_table[None, :]
    return jnp.concatenate([jnp.cos(angles), jnp.sin(angles)], axis=1).astype(BF16)


def silu_grad(values):
    sigmoid_v = jax.nn.sigmoid(values)
    return sigmoid_v * (1.0 + values * (1.0 - sigmoid_v))


def by_chip(grad):
    return grad.reshape(ZS, TWO, TWO, grad.shape[0] // CHIPS, WIDTH)


WGRAD_PIECES = (((0, 0, 184, 0),), ((0, 176, 184, 0),))
EMBED_PIECES = (
    ((0, 0, 16, 0), (1, 0, 16, 16), (2, 0, 128, 32), (6, 0, 8, 160), (3, 0, 24, 168)),
    ((3, 24, 48, 0), (4, 0, 72, 48), (5, 0, 72, 120)),
)


def solution(mesh):
    row_split = P(AXIS)
    row_matrix = P(AXIS, None)
    col_matrix = P(None, AXIS)
    embed_specs = (P(None, None), P(None), P(None, None), P(None)) * 3
    in_specs = (row_split, row_split, row_matrix) + embed_specs + (col_matrix, row_split, row_matrix)
    out_specs = (row_matrix, col_matrix, row_split) + embed_specs

    def local_step(timesteps, guidance, pooled, time_w1, time_b1, time_w2, time_b2, guide_w1, guide_b1, guide_w2, guide_b2, text_w1, text_b1, text_w2, text_b2, w_mod, b_mod, d_mods):
        me = lax.axis_index(AXIS)
        freq_width = time_w1.shape[0]
        inputs_list = [sinusoid(timesteps, freq_width), sinusoid(guidance, freq_width), pooled]
        first, second = [time_w1, guide_w1, text_w1], [time_w2, guide_w2, text_w2]
        count = len(first)
        biases = jnp.stack([time_b1, guide_b1, text_b1, time_b2, guide_b2, text_b2]).astype(F32)
        extra = jnp.pad(b_mod[None, :], ((0, PADDED - SHARE - 1), (0, WIDTH - SHARE)))
        block = jnp.concatenate([w_mod.T, extra], axis=0)
        gathered, part_wgrad, part_bgrad, cond_vec, cond_silu, *rest = gather_blocks(block, d_mods, biases, inputs_list, first, second)
        acts, hidden = rest[:count], rest[count:]
        gathered = gathered.reshape(DEVICES, PADDED, WIDTH)
        full_b = gathered[:, SHARE, :SHARE].reshape(1, MOD).astype(F32)
        wgrad, sums, full_wt, *grads = scatter_sum(by_chip(part_wgrad), d_mods, gathered, cond_vec, hidden, second, inputs_list, acts, WGRAD_PIECES)
        grad_wmod = lax.dynamic_slice(wgrad, (4 * lax.rem(me, TWO), 0), (SHARE, WIDTH)).T
        bgrad_rows = MOD // WIDTH
        part_bgrad = part_bgrad.reshape(bgrad_rows, WIDTH)
        vectors = jnp.concatenate([sums[:ZS], part_bgrad], axis=0)
        vectors = jnp.pad(vectors, ((0, 128 - vectors.shape[0]), (0, 0)))
        sources = [by_chip(g) for g in (*grads, vectors)]
        total, modulation = reduce_all(sources, EMBED_PIECES, cond_silu, full_wt, full_b)
        modulation, *full = unpack(total, modulation, sources, EMBED_PIECES)
        *full, sums = [g.reshape(-1, WIDTH) for g in full]
        grad_bmod = lax.dynamic_slice(sums[ZS:ZS + bgrad_rows].reshape(MOD), (SHARE * me,), (SHARE,))
        embed_grads = [g for i in range(count) for g in (full[i], sums[i], full[i + count], sums[count])]
        return (modulation, grad_wmod, grad_bmod, *embed_grads)

    return jax.shard_map(local_step, mesh=mesh, in_specs=in_specs, out_specs=out_specs, check_vma=False)
```
